512 devices in a mesh: gx: 32 (over y_lo, z, core), gy: 16 (over x, y_hi).
Axes of the slice: x: 4, y: 8 (y_hi: 4, y_lo: 2; y = y_hi * 2 + y_lo), z: 8, core: 2. Of those that a mesh axis runs over, the one named last changes fastest.
Arguments:
- displacement: float32 [3, 256, 128, 128], P(None, 'gx', 'gy'), may hold values from -6 to 6
- velocity: float32 [3, 256, 128, 128], P(None, 'gx', 'gy'), may hold values from -6 to 6
- region: int32 [256, 128, 128], P('gx', 'gy'), may hold values from 0 to 3
- bond_words: int32 [11, 256, 128, 128], P(None, 'gx', 'gy'), may hold values from 0 to 4095, as said below
- moduli: float32 [3, 4], replicated, may hold values from 0.5 to 2
Outputs:
- new_displacement: float32 [3, 256, 128, 128], P(None, 'gx', 'gy')
- new_velocity: float32 [3, 256, 128, 128], P(None, 'gx', 'gy')
The draws below stay inside these ranges and needn't reach their ends.
Inputs may be any that keep to these rules, and one draw needn't show every extreme that they name: `bond_words`: bonds are the integer offsets (a, b, c) with 0 < a*a + b*b + c*c <= 9, numbered 0 to 121 in increasing lexicographic order. Bond q of a node is bit q % 12 of word q // 12 (bit 0 the lowest); a set bit means the bond is intact. A bond whose far end lies outside the grid is never intact; the six bonds of length one are intact wherever they stay inside the grid; bond q of node p equals bond 121 - q of node p + xi_q.
All inputs are finite; a program needn't handle non-finite values.
Results may differ from the reference program's by a relative error of at most 0.00002.
Values sent between devices are 32-bit elements; how exact they have to be, the bound alone decides.
No kernel may reach another device: no remote copies, remote signals or barrier semaphores. Data moves between devices by JAX's collectives and lax.ppermute only.
A program may use at most 64 MiB of HBM per device.

```python
import math
import jax
import jax.numpy as jnp
from jax import lax

HORIZON = 3
REGIONS = 4
STEPS = 1
NX = 256
NY = 128
NZ = 128


bits_per_word = 12


def bond_offsets_drawn():
    listed = []
    for shift_x in range(-HORIZON, HORIZON + 1):
        for shift_y in range(-HORIZON, HORIZON + 1):
            for shift_z in range(-HORIZON, HORIZON + 1):
                radius = shift_x * shift_x + shift_y * shift_y + shift_z * shift_z
                if 0 < radius <= HORIZON * HORIZON:
                    listed.append((shift_x, shift_y, shift_z))
    return listed


def draw_bond_words(key, part):
    offsets = bond_offsets_drawn()
    bond_count = len(offsets)
    word_count = (bond_count + bits_per_word - 1) // bits_per_word
    grid_x = lax.broadcasted_iota(jnp.int32, (NX, NY, NZ), 0)
    grid_y = lax.broadcasted_iota(jnp.int32, (NX, NY, NZ), 1)
    grid_z = lax.broadcasted_iota(jnp.int32, (NX, NY, NZ), 2)
    packed = [jnp.zeros((NX, NY, NZ), jnp.int32) for position in range(word_count)]
    for number, offset in enumerate(offsets):
        shift_x, shift_y, shift_z = offset
        partner = min(number, bond_count - 1 - number)
        sampled = jax.random.randint(jax.random.fold_in(key, 1000 + partner), (NX, NY, NZ), 0, 100) < 86
        if number > partner:
            sampled = jnp.roll(sampled, (-shift_x, -shift_y, -shift_z), axis=(0, 1, 2))
        if shift_x * shift_x + shift_y * shift_y + shift_z * shift_z == 1:
            sampled = jnp.ones_like(sampled)
        inside = (grid_x + shift_x >= 0) & (grid_x + shift_x < NX)
        inside = inside & (grid_y + shift_y >= 0) & (grid_y + shift_y < NY)
        inside = inside & (grid_z + shift_z >= 0) & (grid_z + shift_z < NZ)
        bit_value = (sampled & inside).astype(jnp.int32)
        word_index = number // bits_per_word
        bit_shift = number % bits_per_word
        packed[word_index] = packed[word_index] + jnp.left_shift(bit_value, bit_shift)
    return jnp.stack(packed)


def set_ends(values, own_key, smallest, high):
    spot = [jax.random.randint(jax.random.fold_in(own_key, axis), (), 0, length) for axis, length in enumerate(values.shape)]
    main_axis = values.shape.index(max(values.shape))
    next_to = spot[:main_axis] + [(spot[main_axis] + 1) % values.shape[main_axis]] + spot[main_axis + 1:]
    return values.at[tuple(spot)].set(smallest).at[tuple(next_to)].set(high)


def level_of(key, dims, split, low, largest):
    gain = 1.0
    for dim, blocks in split:
        draws = jax.random.uniform(jax.random.fold_in(jax.random.fold_in(key, 6), dim), (blocks,), jnp.float32, low / len(split), largest / len(split))
        gain = gain * jnp.repeat(jnp.exp(draws), dims[dim] // blocks).reshape((-1,) + (1,) * (len(dims) - 1 - dim))
    return gain


def centred(stream_key, extent, deviation, limit, shards=(), dtype=jnp.bfloat16):
    values = jax.random.normal(stream_key, extent, jnp.float32) * deviation
    if len(shards) > 0:
        values = level_of(stream_key, extent, shards, -0.22, 0.18) * values
    return jnp.clip(values, min=-limit, max=limit).astype(dtype)


def setup_inputs(seed: int = 0) -> dict:
    splits = jax.random.split(jax.random.key(seed), 6)
    return {
        "displacement": centred(splits[0], (3, NX, NY, NZ), 1.0, 6.0, ((1, 32), (2, 16)), jnp.float32),
        "velocity": centred(splits[1], (3, NX, NY, NZ), 1.0, 6.0, ((1, 32), (2, 16)), jnp.float32),
        "region": set_ends(jax.random.randint(splits[2], (NX, NY, NZ), 0, REGIONS), jax.random.fold_in(splits[2], 1), 0, REGIONS - 1).astype(jnp.int32),
        "bond_words": draw_bond_words(jax.random.fold_in(splits[5], 71), 0),
        "moduli": jnp.clip(jnp.exp(jax.random.uniform(splits[4], (3, REGIONS), jnp.float32, math.log(0.5), math.log(2.0))), 0.5, 2.0),
    }


time_step = 0.3
bits_per_word = 12

def bond_offsets():
    listed = []
    for shift_x in range(-HORIZON, HORIZON + 1):
        for shift_y in range(-HORIZON, HORIZON + 1):
            for shift_z in range(-HORIZON, HORIZON + 1):
                radius = shift_x * shift_x + shift_y * shift_y + shift_z * shift_z
                if 0 < radius <= HORIZON * HORIZON:
                    listed.append((shift_x, shift_y, shift_z))
    return listed

def bond_length(offset):
    return math.sqrt(offset[0] * offset[0] + offset[1] * offset[1] + offset[2] * offset[2])

def bond_bit(bond_words, number):
    word_index = number // bits_per_word
    bit_shift = number % bits_per_word
    return jnp.bitwise_and(jnp.right_shift(bond_words[word_index], bit_shift), 1).astype(jnp.float32)

def materials(region, moduli):
    fields = jnp.zeros((3,) + region.shape, jnp.float32)
    for material in range(moduli.shape[1]):
        fields = jnp.where((region == material)[None], moduli[:, material][:, None, None, None], fields)
    return (fields[0], fields[1], fields[2])

def window(padded, offset, block_shape):
    start_x = HORIZON + offset[0]
    start_y = HORIZON + offset[1]
    start_z = HORIZON + offset[2]
    return padded[..., start_x:start_x + block_shape[0], start_y:start_y + block_shape[1], start_z:start_z + block_shape[2]]

def stretch_of(padded, centre, offset):
    length = bond_length(offset)
    neighbour = window(padded, offset, centre.shape[1:])
    along = (neighbour[0] - centre[0]) * (offset[0] / length)
    along = along + (neighbour[1] - centre[1]) * (offset[1] / length)
    return along + (neighbour[2] - centre[2]) * (offset[2] / length)

def reference(displacement, velocity, region, bond_words, moduli):
    offsets = bond_offsets()
    block_shape = region.shape
    bulk_modulus, shear_modulus, density = materials(region, moduli)
    volume = jnp.zeros(block_shape, jnp.float32)
    for number, offset in enumerate(offsets):
        volume = volume + bond_bit(bond_words, number) * bond_length(offset)
    pressure_ratio = (3.0 * bulk_modulus - 5.0 * shear_modulus) / volume
    shear_term = 15.0 * shear_modulus / volume
    inverse_mass = 1.0 / density
    margins = ((HORIZON, HORIZON),) * 3
    shear_padded = jnp.pad(shear_term, margins)
    for iteration in range(STEPS):
        padded = jnp.pad(displacement, ((0, 0),) + margins)
        accumulated = jnp.zeros(block_shape, jnp.float32)
        for number, offset in enumerate(offsets):
            accumulated = accumulated + bond_bit(bond_words, number) * stretch_of(padded, displacement, offset)
        dilatation = 3.0 * accumulated / volume
        pressure_term = dilatation * pressure_ratio
        pressure_padded = jnp.pad(pressure_term, margins)
        force_parts = [jnp.zeros(block_shape, jnp.float32) for position in range(3)]
        for number, offset in enumerate(offsets):
            length = bond_length(offset)
            stretch = stretch_of(padded, displacement, offset)
            coefficient = bond_bit(bond_words, number) * (pressure_term + window(pressure_padded, offset, block_shape) + (shear_term + window(shear_padded, offset, block_shape)) * stretch * (1.0 / length))
            for position in range(3):
                force_parts[position] = force_parts[position] + coefficient * (offset[position] / length)
        force_sum = jnp.stack(force_parts)
        velocity = velocity + time_step * force_sum * inverse_mass
        displacement = displacement + time_step * velocity
    return (displacement, velocity)
```

```python
import math

import jax
import jax.numpy as jnp
from jax import lax
from jax.experimental import pallas as pl
from jax.experimental.pallas import tpu as pltpu
from jax.sharding import PartitionSpec as P

HORIZON = 3
time_step = 0.3
bits_per_word = 12
F32 = jnp.float32
LANES = 128

OFFSETS = [
    (a, b, c)
    for a in range(-HORIZON, HORIZON + 1)
    for b in range(-HORIZON, HORIZON + 1)
    for c in range(-HORIZON, HORIZON + 1)
    if 0 < a * a + b * b + c * c <= HORIZON * HORIZON
]
CLASSES = sorted({a * a + b * b + c * c for a, b, c in OFFSETS})
WORDS = (len(OFFSETS) + bits_per_word - 1) // bits_per_word


def square(offset):
    return offset[0] * offset[0] + offset[1] * offset[1] + offset[2] * offset[2]


SU = 14
SW = 9
SH = 7
SP = 9
BLOCKS = (-3, 5)
SLAB = 54


def rolled(value, shift):
    return value if shift == 0 else pltpu.roll(value, (-shift) % LANES, 1)


def u_at(ref, component, shift, x, y):
    return ref[component * 7 + shift + 3, pl.ds((x + 8) * SU + y + 3, 8, stride=SU), :]


def word_at(ref, k, x, y):
    return ref[k, pl.ds((x + 8) * SW + y, 8, stride=SW), :]


def uh_at(ref, component, shift, x, h):
    return ref[component * 7 + shift + 3, pl.ds((x + 5) * SH + h, 8, stride=SH), :]


def scaled(value, factor):
    if factor == 1:
        return value
    if factor == -1:
        return -value
    return value * float(factor)


def combined(values, offset):
    total = None
    for value, factor in zip(values, offset):
        if factor == 0:
            continue
        if total is None:
            total = scaled(value, factor)
        elif factor == 1:
            total = total + value
        elif factor == -1:
            total = total - value
        else:
            total = total + value * float(factor)
    return total


def bit(word, number):
    return (word & (1 << (number % bits_per_word))) != 0


def add_to(store, key, value):
    store[key] = value if store.get(key) is None else store[key] + value


def by_class(store):
    total = None
    for cls, value in store.items():
        term = value * (1.0 / math.sqrt(cls))
        total = term if total is None else total + term
    return total


def chosen(region, moduli_ref, row):
    value = jnp.where(region == 1, moduli_ref[row, 1], moduli_ref[row, 0])
    value = jnp.where(region == 2, moduli_ref[row, 2], value)
    return jnp.where(region == 3, moduli_ref[row, 3], value)


def crossing(y):
    found = []
    for number, offset in enumerate(OFFSETS):
        target = y + offset[1]
        if target < 0:
            found.append((number, offset, target + 3))
        elif target > 7:
            found.append((number, offset, target - 8 + 3))
    return found


def slabs_x(u_ref, w_ref, r_ref, even_ref, odd_ref):
    parity = lax.axis_index("gx") % 2
    for ref, right in ((even_ref, 1 - parity), (odd_ref, parity)):
        w_start = right * 5
        u_start = right * 2
        for k in range(WORDS):
            for d in range(3):
                ref[k * 3 + d] = w_ref[k, w_start + d].astype(F32)
        for c in range(3):
            for d in range(6):
                ref[33 + c * 6 + d] = u_ref[c, u_start + d]
        for d in range(3):
            ref[51 + d] = r_ref[w_start + d].astype(F32)


def halves(even_ref, odd_ref, parity, tile_left, tile_right, y):
    def pick(tile, left):
        rows = pl.ds(tile * 8 + y, 8, stride=8)
        even, odd = (even_ref[rows, :], odd_ref[rows, :])
        return jnp.where(parity == 0, odd, even) if left else jnp.where(parity == 0, even, odd)

    return pick(tile_left, True), pick(tile_right, False)


def slabs_y(u_ref, even_ref, odd_ref, down_ref, up_ref):
    parity = lax.axis_index("gx") % 2
    for ref, first in ((down_ref, 0), (up_ref, 5)):
        for c in range(3):
            for d in range(3):
                y = first + d
                j = c * 3 + d
                left, right = halves(
                    even_ref, odd_ref, parity, 33 + c * 6 + 1, 33 + c * 6 - 3, y
                )
                ref[pl.ds(j, 8, stride=9), :] = left
                ref[pl.ds(10 * 9 + j, 8, stride=9), :] = right
                ref[pl.ds(5 * 9 + j, 8, stride=9), :] = u_ref[
                    pl.ds(c * 64 + y, 8, stride=8), :
                ]


def inner_dilatation(
    u_ref, w_ref, r_ref, moduli_ref, even_ref, odd_ref, ux_ref, wx_ref, out_ref
):
    parity = lax.axis_index("gx") % 2
    zero = jnp.zeros((8, LANES), F32)
    for y in (-3, -2, -1, 8, 9, 10):
        for lead in range(21):
            for x in (-8, 0, 8):
                ux_ref[lead, pl.ds((x + 8) * SU + y + 3, 8, stride=SU), :] = zero
    for y in range(8):
        for c in range(3):
            left, right = halves(even_ref, odd_ref, parity, 33 + c * 6 - 2, 33 + c * 6, y)
            own = u_ref[pl.ds(c * 64 + y, 8, stride=8), :]
            for x, value in ((-8, left), (8, right), (0, own)):
                for shift in range(-3, 4):
                    ux_ref[
                        c * 7 + shift + 3, pl.ds((x + 8) * SU + y + 3, 8, stride=SU), :
                    ] = rolled(value, shift)
        for k in range(WORDS + 1):
            if k < WORDS:
                left, right = halves(even_ref, odd_ref, parity, k * 3, k * 3, y)
                own = w_ref[pl.ds(k * 64 + y, 8, stride=8), :]
                places = (-3, 8)
            else:
                left, right = halves(even_ref, odd_ref, parity, 46, 46, y)
                own = r_ref[pl.ds(y, 8, stride=8), :]
                places = (-8, 3)
            for x, value in (
                (places[0], left.astype(jnp.int32)),
                (places[1], right.astype(jnp.int32)),
                (0, own),
            ):
                wx_ref[k, pl.ds((x + 8) * SW + y, 8, stride=SW), :] = value

    for index, x0 in enumerate(BLOCKS):

        def row(y, carry, index=index, x0=x0):
            own = [u_at(ux_ref, c, 0, x0, y) for c in range(3)]
            sums = {}
            counts = {}
            word = None
            for number, offset in enumerate(OFFSETS):
                if number % bits_per_word == 0:
                    k = number // bits_per_word
                    word = word_at(wx_ref, k, x0, y)
                    for cls in CLASSES:
                        held = 0
                        for other in range(
                            number, min(number + bits_per_word, len(OFFSETS))
                        ):
                            if square(OFFSETS[other]) == cls:
                                held |= 1 << (other - number)
                        if held:
                            add_to(counts, cls, lax.population_count(word & held))
                difference = [
                    u_at(ux_ref, c, offset[2], x0 + offset[0], y + offset[1]) - own[c]
                    if offset[c] != 0
                    else None
                    for c in range(3)
                ]
                along = combined(difference, offset)
                add_to(
                    sums, square(offset), jnp.where(bit(word, number), along, 0.0)
                )
            volume = None
            for cls in CLASSES:
                term = counts[cls].astype(F32) * math.sqrt(cls)
                volume = term if volume is None else volume + term
            inverse = 1.0 / jnp.where(volume > 0.0, volume, 1.0)
            region = word_at(wx_ref, WORDS, x0, y)
            bulk = chosen(region, moduli_ref, 0)
            shear = chosen(region, moduli_ref, 1)
            out_ref[index * 8 + y] = by_class(sums)
            out_ref[16 + index * 8 + y] = (3.0 * inverse) * (
                (3.0 * bulk - 5.0 * shear) * inverse
            )
            out_ref[32 + index * 8 + y] = 15.0 * shear * inverse
            return carry

        lax.fori_loop(0, 8, row, 0)


def outer_dilatation(
    below_ref, above_ref, wx_ref, part_ref, uh_ref, ps_ref, down_ref, up_ref
):
    for side, ref in enumerate((below_ref, above_ref)):
        for c in range(3):
            for d in range(3):
                for x in (-5, 3, 5):
                    value = ref[pl.ds((x + 5) * 9 + c * 3 + d, 8, stride=9), :]
                    for shift in range(-3, 4):
                        uh_ref[
                            c * 7 + shift + 3,
                            pl.ds((x + 5) * SH + side * 3 + d, 8, stride=SH),
                            :,
                        ] = rolled(value, shift)
    for y in range(8):
        for index, x0 in enumerate(BLOCKS):
            total = part_ref[index * 8 + y]
            sums = {}
            word = None
            loaded = -1
            for number, offset, h in crossing(y):
                if number // bits_per_word != loaded:
                    loaded = number // bits_per_word
                    word = word_at(wx_ref, loaded, x0, y)
                far = [
                    uh_at(uh_ref, c, offset[2], x0 + offset[0], h) if offset[c] != 0 else None
                    for c in range(3)
                ]
                add_to(
                    sums,
                    square(offset),
                    jnp.where(bit(word, number), combined(far, offset), 0.0),
                )
            if sums:
                total = total + by_class(sums)
            rows = pl.ds((x0 + 3) * SP + y, 8, stride=SP)
            ps_ref[0, rows, :] = total * part_ref[16 + index * 8 + y]
            ps_ref[1, rows, :] = part_ref[32 + index * 8 + y]
    for ref, first in ((down_ref, 0), (up_ref, 5)):
        for field in range(2):
            for d in range(3):
                for x in (-2, 2):
                    ref[pl.ds((x + 2) * 6 + field * 3 + d, 8, stride=6), :] = ps_ref[
                        field, pl.ds((x + 3) * SP + first + d, 8, stride=SP), :
                    ]


def px_at(ref, field, shift, x, y):
    return ref[field * 7 + shift + 3, pl.ds((x + 3) * SU + y + 3, 8, stride=SU), :]


def inner_force(ux_ref, wx_ref, ps_ref, out_ref, px_ref):
    zero = jnp.zeros((8, LANES), F32)
    for field in range(2):
        for x in BLOCKS:
            for y in (-3, -2, -1, 8, 9, 10):
                for lead in range(7):
                    px_ref[
                        field * 7 + lead, pl.ds((x + 3) * SU + y + 3, 8, stride=SU), :
                    ] = zero
            for y in range(8):
                value = ps_ref[field, pl.ds((x + 3) * SP + y, 8, stride=SP), :]
                for shift in range(-3, 4):
                    px_ref[
                        field * 7 + shift + 3,
                        pl.ds((x + 3) * SU + y + 3, 8, stride=SU),
                        :,
                    ] = rolled(value, shift)

    def row(y, carry):
        own = [u_at(ux_ref, c, 0, 0, y) for c in range(3)]
        pressure = px_at(px_ref, 0, 0, 0, y)
        shear = px_at(px_ref, 1, 0, 0, y)
        force = [None, None, None]
        word = None
        column = {}
        for number, offset in enumerate(OFFSETS):
            if number % bits_per_word == 0:
                word = word_at(wx_ref, number // bits_per_word, 0, y)
            a, b, c = offset
            difference = [
                u_at(ux_ref, i, c, a, y + b) - own[i] if offset[i] != 0 else None
                for i in range(3)
            ]
            along = combined(difference, offset)
            cls = square(offset)
            value = (pressure + px_at(px_ref, 0, c, a, y + b)) + (
                shear + px_at(px_ref, 1, c, a, y + b)
            ) * (along * (1.0 / cls))
            column[c] = jnp.where(
                bit(word, number), value * (1.0 / math.sqrt(cls)), 0.0
            )
            last = number + 1 == len(OFFSETS) or OFFSETS[number + 1][:2] != (a, b)
            if last:
                force = fold(force, column, a, b)
                column = {}
        for i in range(3):
            out_ref[i * 8 + y] = force[i]
        return carry

    lax.fori_loop(0, 8, row, 0)


def fold(force, column, a, b):
    force = list(force)
    total = None
    for value in column.values():
        total = value if total is None else total + value
    for i, factor in ((0, a), (1, b)):
        if factor != 0:
            term = scaled(total, factor)
            force[i] = term if force[i] is None else force[i] + term
    for c, value in column.items():
        if c > 0:
            term = scaled(value - column[-c], c)
            force[2] = term if force[2] is None else force[2] + term
    return force


def outer_force(
    below_ref,
    above_ref,
    ux_ref,
    uh_ref,
    wx_ref,
    ps_ref,
    part_ref,
    u_ref,
    v_ref,
    moduli_ref,
    new_u_ref,
    new_v_ref,
    ph_ref,
):
    for side, ref in enumerate((below_ref, above_ref)):
        for field in range(2):
            for d in range(3):
                for x in (-2, 2):
                    value = ref[pl.ds((x + 2) * 6 + field * 3 + d, 8, stride=6), :]
                    for shift in range(-3, 4):
                        ph_ref[
                            field * 7 + shift + 3,
                            pl.ds((x + 2) * SH + side * 3 + d, 8, stride=SH),
                            :,
                        ] = rolled(value, shift)
    for y in range(8):
        force = [part_ref[i * 8 + y] for i in range(3)]
        own = [u_at(ux_ref, c, 0, 0, y) for c in range(3)]
        shear = ps_ref[1, pl.ds(3 * SP + y, 8, stride=SP), :]
        column = {}
        bonds = crossing(y)
        loaded = -1
        word = None
        for position, (number, offset, h) in enumerate(bonds):
            if number // bits_per_word != loaded:
                loaded = number // bits_per_word
                word = word_at(wx_ref, loaded, 0, y)
            a, b, c = offset
            cls = square(offset)
            far = [
                uh_at(uh_ref, i, c, a, h) if offset[i] != 0 else None for i in range(3)
            ]
            reach = combined(far, offset)
            along = combined(
                [far[i] - own[i] if offset[i] != 0 else None for i in range(3)], offset
            )
            rows = pl.ds((a + 2) * SH + h, 8, stride=SH)
            far_pressure = ph_ref[c + 3, rows, :]
            far_shear = ph_ref[7 + c + 3, rows, :]
            value = far_pressure + (far_shear * along + shear * reach) * (1.0 / cls)
            column[c] = jnp.where(
                bit(word, number), value * (1.0 / math.sqrt(cls)), 0.0
            )
            if position + 1 == len(bonds) or bonds[position + 1][1][:2] != (a, b):
                force = fold(force, column, a, b)
                column = {}
        density = chosen(word_at(wx_ref, WORDS, 0, y), moduli_ref, 2)
        step = time_step / density
        for i in range(3):
            rows = pl.ds(i * 64 + y, 8, stride=8)
            velocity = v_ref[rows, :] + force[i] * step
            new_v_ref[rows, :] = velocity
            new_u_ref[rows, :] = u_ref[rows, :] + time_step * velocity


def call(body, name, outs, args, scalars=(), scratch=(), flops=1000):
    vmem = pl.BlockSpec(memory_space=pltpu.VMEM)
    smem = pl.BlockSpec(memory_space=pltpu.SMEM)
    return pl.pallas_call(
        body,
        name=name,
        out_shape=[jax.ShapeDtypeStruct(shape, dtype) for shape, dtype in outs],
        in_specs=[smem if position in scalars else vmem for position in range(len(args))],
        out_specs=[vmem for _ in outs],
        scratch_shapes=[pltpu.VMEM(shape, dtype) for shape, dtype in scratch],
        cost_estimate=pl.CostEstimate(flops=flops, bytes_accessed=100000, transcendentals=0),
        compiler_params=pltpu.CompilerParams(vmem_limit_bytes=16 * 1024 * 1024),
    )(*args)


def along_y(down, up):
    size = lax.axis_size("gy")
    upward = [(i, i + 1) for i in range(size - 1)]
    downward = [(i + 1, i) for i in range(size - 1)]
    below = lax.ppermute(up, "gy", upward)
    above = lax.ppermute(down, "gy", downward)
    return below, above


def on_device(displacement, velocity, region, bond_words, moduli):
    even, odd = call(
        slabs_x,
        "slabs_x",
        [((SLAB, 8, LANES), F32)] * 2,
        (displacement, bond_words, region),
    )
    size = lax.axis_size("gx")
    even = lax.ppermute(even, "gx", [(i, i ^ 1) for i in range(size)])
    odd = lax.ppermute(
        odd, "gx", [(i, ((i - 1) ^ 1) + 1) for i in range(1, size - 1)]
    )
    even = even.reshape(SLAB * 8, LANES)
    odd = odd.reshape(SLAB * 8, LANES)
    u = displacement.reshape(192, LANES)
    down, up = call(slabs_y, "slabs_y", [((162, LANES), F32)] * 2, (u, even, odd))
    below, above = along_y(down, up)
    ux, wx, part = call(
        inner_dilatation,
        "inner_dilatation",
        [((21, 24 * SU, LANES), F32), ((12, 24 * SW, LANES), jnp.int32), ((48, 8, LANES), F32)],
        (u, bond_words.reshape(704, LANES), region.reshape(64, LANES), moduli, even, odd),
        scalars=(3,),
        flops=40_000_000,
    )
    uh, ps, down, up = call(
        outer_dilatation,
        "outer_dilatation",
        [
            ((21, 20 * SH, LANES), F32),
            ((2, 16 * SP, LANES), F32),
            ((72, LANES), F32),
            ((72, LANES), F32),
        ],
        (below, above, wx, part),
        flops=4_000_000,
    )
    below, above = along_y(down, up)
    (force,) = call(
        inner_force,
        "inner_force",
        [((24, 8, LANES), F32)],
        (ux, wx, ps),
        scratch=[((14, 16 * SU, LANES), F32)],
        flops=40_000_000,
    )
    new_u, new_v = call(
        outer_force,
        "outer_force",
        [((192, LANES), F32)] * 2,
        (below, above, ux, uh, wx, ps, force, u, velocity.reshape(192, LANES), moduli),
        scalars=(9,),
        scratch=[((14, 12 * SH, LANES), F32)],
        flops=4_000_000,
    )
    return new_u.reshape(displacement.shape), new_v.reshape(velocity.shape)


def solution(mesh):
    placed = (
        P(None, "gx", "gy", None),
        P(None, "gx", "gy", None),
        P("gx", "gy", None),
        P(None, "gx", "gy", None),
        P(),
    )
    return jax.shard_map(
        on_device,
        mesh=mesh,
        in_specs=placed,
        out_specs=(P(None, "gx", "gy", None), P(None, "gx", "gy", None)),
        check_vma=False,
    )
```

```python
import math

import jax
import jax.numpy as jnp
from jax import lax
from jax.experimental import pallas as pl
from jax.experimental.pallas import tpu as pltpu
from jax.sharding import PartitionSpec as P


HORIZON = 3
time_step = 0.3
bits_per_word = 12
F32 = jnp.float32
LANES = 128

OFFSETS = [
    (a, b, c)
    for a in range(-HORIZON, HORIZON + 1)
    for b in range(-HORIZON, HORIZON + 1)
    for c in range(-HORIZON, HORIZON + 1)
    if 0 < a * a + b * b + c * c <= HORIZON * HORIZON
]
CLASSES = sorted({a * a + b * b + c * c for a, b, c in OFFSETS})
WORDS = (len(OFFSETS) + bits_per_word - 1) // bits_per_word


def square(offset):
    return offset[0] * offset[0] + offset[1] * offset[1] + offset[2] * offset[2]


SU = 14
SW = 9
SH = 7
SP = 9
BLOCKS = (-3, 5)
SLAB = 54


def rolled(value, shift):
    return value if shift == 0 else pltpu.roll(value, (-shift) % LANES, 1)


def u_at(ref, component, shift, x, y):
    return ref[component * 7 + shift + 3, pl.ds((x + 8) * SU + y + 3, 8, stride=SU), :]


def word_at(ref, k, x, y):
    return ref[k, pl.ds((x + 8) * SW + y, 8, stride=SW), :]


def uh_at(ref, component, shift, x, h):
    return ref[component * 7 + shift + 3, pl.ds((x + 5) * SH + h, 8, stride=SH), :]


def scaled(value, factor):
    if factor == 1:
        return value
    if factor == -1:
        return -value
    return value * float(factor)


def combined(values, offset):
    total = None
    for value, factor in zip(values, offset):
        if factor == 0:
            continue
        if total is None:
            total = scaled(value, factor)
        elif factor == 1:
            total = total + value
        elif factor == -1:
            total = total - value
        else:
            total = total + value * float(factor)
    return total


def bit(word, number):
    return (word & (1 << (number % bits_per_word))) != 0


def add_to(store, key, value):
    store[key] = value if store.get(key) is None else store[key] + value


def by_class(store):
    total = None
    for cls, value in store.items():
        term = value * (1.0 / math.sqrt(cls))
        total = term if total is None else total + term
    return total


def chosen(region, moduli_ref, row):
    value = jnp.where(region == 1, moduli_ref[row, 1], moduli_ref[row, 0])
    value = jnp.where(region == 2, moduli_ref[row, 2], value)
    return jnp.where(region == 3, moduli_ref[row, 3], value)


def crossing(y):
    found = []
    for number, offset in enumerate(OFFSETS):
        target = y + offset[1]
        if target < 0:
            found.append((number, offset, target + 3))
        elif target > 7:
            found.append((number, offset, target - 8 + 3))
    return found


def slabs_x(
    u_hbm, w_hbm, r_hbm, odd_ref, even_ref, u_ref, w_ref, r_ref, u_sem, w_sem, r_sem
):
    parity = lax.axis_index("gx") % 2
    copies = [
        pltpu.make_async_copy(w_hbm, w_ref, w_sem),
        pltpu.make_async_copy(u_hbm, u_ref, u_sem),
        pltpu.make_async_copy(r_hbm, r_ref, r_sem),
    ]
    for copy in copies:
        copy.start()
    for copy in copies:
        copy.wait()
    for ref, right in ((even_ref, 1 - parity), (odd_ref, parity)):
        w_start = right * 5
        u_start = right * 2
        for k in range(WORDS):
            for d in range(3):
                ref[k * 3 + d] = w_ref[k, w_start + d].astype(F32)
        for c in range(3):
            for d in range(6):
                ref[33 + c * 6 + d] = u_ref[c, u_start + d]
        for d in range(3):
            ref[51 + d] = r_ref[w_start + d].astype(F32)


def halves(even_ref, odd_ref, parity, tile_left, tile_right, y):
    def pick(tile, left):
        rows = pl.ds(tile * 8 + y, 8, stride=8)
        even, odd = (even_ref[rows, :], odd_ref[rows, :])
        return jnp.where(parity == 0, odd, even) if left else jnp.where(parity == 0, even, odd)

    return pick(tile_left, True), pick(tile_right, False)


def slabs_y(u_ref, even_ref, odd_ref, down_ref, up_ref):
    parity = lax.axis_index("gx") % 2
    for ref, first in ((down_ref, 0), (up_ref, 5)):
        for c in range(3):
            for d in range(3):
                y = first + d
                j = c * 3 + d
                left, right = halves(
                    even_ref, odd_ref, parity, 33 + c * 6 + 1, 33 + c * 6 - 3, y
                )
                ref[pl.ds(j, 8, stride=9), :] = left
                ref[pl.ds(10 * 9 + j, 8, stride=9), :] = right
                ref[pl.ds(5 * 9 + j, 8, stride=9), :] = u_ref[
                    pl.ds(c * 64 + y, 8, stride=8), :
                ]


def inner_dilatation(
    u_ref,
    w_ref,
    r_ref,
    moduli_hbm,
    even_ref,
    odd_ref,
    ux_ref,
    wx_ref,
    out_ref,
    step_ref,
    moduli_ref,
    moduli_sem,
):
    fetch = pltpu.make_async_copy(moduli_hbm, moduli_ref, moduli_sem)
    fetch.start()
    parity = lax.axis_index("gx") % 2
    zero = jnp.zeros((8, LANES), F32)
    for y in (-3, -2, -1, 8, 9, 10):
        for lead in range(21):
            for x in (-8, 0, 8):
                ux_ref[lead, pl.ds((x + 8) * SU + y + 3, 8, stride=SU), :] = zero
    for y in range(8):
        for c in range(3):
            left, right = halves(even_ref, odd_ref, parity, 33 + c * 6 - 2, 33 + c * 6, y)
            own = u_ref[pl.ds(c * 64 + y, 8, stride=8), :]
            for x, value in ((-8, left), (8, right), (0, own)):
                for shift in range(-3, 4):
                    ux_ref[
                        c * 7 + shift + 3, pl.ds((x + 8) * SU + y + 3, 8, stride=SU), :
                    ] = rolled(value, shift)
        for k in range(WORDS + 1):
            if k < WORDS:
                left, right = halves(even_ref, odd_ref, parity, k * 3, k * 3, y)
                own = w_ref[pl.ds(k * 64 + y, 8, stride=8), :]
                places = (-3, 8)
            else:
                left, right = halves(even_ref, odd_ref, parity, 46, 46, y)
                own = r_ref[pl.ds(y, 8, stride=8), :]
                places = (-8, 3)
            for x, value in (
                (places[0], left.astype(jnp.int32)),
                (places[1], right.astype(jnp.int32)),
                (0, own),
            ):
                wx_ref[k, pl.ds((x + 8) * SW + y, 8, stride=SW), :] = value

    fetch.wait()
    for y in range(8):
        region = r_ref[pl.ds(y, 8, stride=8), :]
        step_ref[y] = time_step / chosen(region, moduli_ref, 2)
    for index, x0 in enumerate(BLOCKS):

        def row(y, carry, index=index, x0=x0):
            own = [u_at(ux_ref, c, 0, x0, y) for c in range(3)]
            sums = {}
            counts = {}
            word = None
            for number, offset in enumerate(OFFSETS):
                if number % bits_per_word == 0:
                    k = number // bits_per_word
                    word = word_at(wx_ref, k, x0, y)
                    for cls in CLASSES:
                        held = 0
                        for other in range(
                            number, min(number + bits_per_word, len(OFFSETS))
                        ):
                            if square(OFFSETS[other]) == cls:
                                held |= 1 << (other - number)
                        if held:
                            add_to(counts, cls, lax.population_count(word & held))
                difference = [
                    u_at(ux_ref, c, offset[2], x0 + offset[0], y + offset[1]) - own[c]
                    if offset[c] != 0
                    else None
                    for c in range(3)
                ]
                along = combined(difference, offset)
                add_to(
                    sums, square(offset), jnp.where(bit(word, number), along, 0.0)
                )
            volume = None
            for cls in CLASSES:
                term = counts[cls].astype(F32) * math.sqrt(cls)
                volume = term if volume is None else volume + term
            inverse = 1.0 / jnp.where(volume > 0.0, volume, 1.0)
            region = word_at(wx_ref, WORDS, x0, y)
            bulk = chosen(region, moduli_ref, 0)
            shear = chosen(region, moduli_ref, 1)
            out_ref[index * 8 + y] = by_class(sums)
            out_ref[16 + index * 8 + y] = (3.0 * inverse) * (
                (3.0 * bulk - 5.0 * shear) * inverse
            )
            out_ref[32 + index * 8 + y] = 15.0 * shear * inverse
            return carry

        lax.fori_loop(0, 8, row, 0)


def outer_dilatation(
    below_ref, above_ref, wx_ref, part_ref, uh_ref, ps_ref, down_ref, up_ref
):
    for side, ref in enumerate((below_ref, above_ref)):
        for c in range(3):
            for d in range(3):
                for x in (-5, 3, 5):
                    value = ref[pl.ds((x + 5) * 9 + c * 3 + d, 8, stride=9), :]
                    for shift in range(-3, 4):
                        uh_ref[
                            c * 7 + shift + 3,
                            pl.ds((x + 5) * SH + side * 3 + d, 8, stride=SH),
                            :,
                        ] = rolled(value, shift)
    for y in range(8):
        for index, x0 in enumerate(BLOCKS):
            total = part_ref[index * 8 + y]
            sums = {}
            word = None
            loaded = -1
            for number, offset, h in crossing(y):
                if number // bits_per_word != loaded:
                    loaded = number // bits_per_word
                    word = word_at(wx_ref, loaded, x0, y)
                far = [
                    uh_at(uh_ref, c, offset[2], x0 + offset[0], h) if offset[c] != 0 else None
                    for c in range(3)
                ]
                add_to(
                    sums,
                    square(offset),
                    jnp.where(bit(word, number), combined(far, offset), 0.0),
                )
            if sums:
                total = total + by_class(sums)
            rows = pl.ds((x0 + 3) * SP + y, 8, stride=SP)
            ps_ref[0, rows, :] = total * part_ref[16 + index * 8 + y]
            ps_ref[1, rows, :] = part_ref[32 + index * 8 + y]
    for ref, first in ((down_ref, 0), (up_ref, 5)):
        for field in range(2):
            for d in range(3):
                for x in (-2, 2):
                    ref[pl.ds((x + 2) * 6 + field * 3 + d, 8, stride=6), :] = ps_ref[
                        field, pl.ds((x + 3) * SP + first + d, 8, stride=SP), :
                    ]


def px_at(ref, field, shift, x, y):
    return ref[field * 7 + shift + 3, pl.ds((x + 3) * SU + y + 3, 8, stride=SU), :]


def inner_force(ux_ref, wx_ref, ps_ref, out_ref, px_ref):
    zero = jnp.zeros((8, LANES), F32)
    for field in range(2):
        for x in BLOCKS:
            for y in (-3, -2, -1, 8, 9, 10):
                for lead in range(7):
                    px_ref[
                        field * 7 + lead, pl.ds((x + 3) * SU + y + 3, 8, stride=SU), :
                    ] = zero
            for y in range(8):
                value = ps_ref[field, pl.ds((x + 3) * SP + y, 8, stride=SP), :]
                for shift in range(-3, 4):
                    px_ref[
                        field * 7 + shift + 3,
                        pl.ds((x + 3) * SU + y + 3, 8, stride=SU),
                        :,
                    ] = rolled(value, shift)

    def row(y, carry):
        own = [u_at(ux_ref, c, 0, 0, y) for c in range(3)]
        pressure = px_at(px_ref, 0, 0, 0, y)
        shear = px_at(px_ref, 1, 0, 0, y)
        force = [None, None, None]
        word = None
        column = {}
        for number, offset in enumerate(OFFSETS):
            if number % bits_per_word == 0:
                word = word_at(wx_ref, number // bits_per_word, 0, y)
            a, b, c = offset
            difference = [
                u_at(ux_ref, i, c, a, y + b) - own[i] if offset[i] != 0 else None
                for i in range(3)
            ]
            along = combined(difference, offset)
            cls = square(offset)
            value = (pressure + px_at(px_ref, 0, c, a, y + b)) + (
                shear + px_at(px_ref, 1, c, a, y + b)
            ) * (along * (1.0 / cls))
            column[c] = jnp.where(
                bit(word, number), value * (1.0 / math.sqrt(cls)), 0.0
            )
            last = number + 1 == len(OFFSETS) or OFFSETS[number + 1][:2] != (a, b)
            if last:
                force = fold(force, column, a, b)
                column = {}
        for i in range(3):
            out_ref[i * 8 + y] = force[i]
        return carry

    lax.fori_loop(0, 8, row, 0)


def fold(force, column, a, b):
    force = list(force)
    total = None
    for value in column.values():
        total = value if total is None else total + value
    for i, factor in ((0, a), (1, b)):
        if factor != 0:
            term = scaled(total, factor)
            force[i] = term if force[i] is None else force[i] + term
    for c, value in column.items():
        if c > 0:
            term = scaled(value - column[-c], c)
            force[2] = term if force[2] is None else force[2] + term
    return force


def outer_force(
    below_ref,
    above_ref,
    ux_ref,
    uh_ref,
    wx_ref,
    ps_ref,
    part_ref,
    u_ref,
    v_ref,
    step_ref,
    new_u_ref,
    new_v_ref,
    ph_ref,
):
    for side, ref in enumerate((below_ref, above_ref)):
        for field in range(2):
            for d in range(3):
                for x in (-2, 2):
                    value = ref[pl.ds((x + 2) * 6 + field * 3 + d, 8, stride=6), :]
                    for shift in range(-3, 4):
                        ph_ref[
                            field * 7 + shift + 3,
                            pl.ds((x + 2) * SH + side * 3 + d, 8, stride=SH),
                            :,
                        ] = rolled(value, shift)
    for y in range(8):
        force = [part_ref[i * 8 + y] for i in range(3)]
        own = [u_at(ux_ref, c, 0, 0, y) for c in range(3)]
        shear = ps_ref[1, pl.ds(3 * SP + y, 8, stride=SP), :]
        column = {}
        bonds = crossing(y)
        loaded = -1
        word = None
        for position, (number, offset, h) in enumerate(bonds):
            if number // bits_per_word != loaded:
                loaded = number // bits_per_word
                word = word_at(wx_ref, loaded, 0, y)
            a, b, c = offset
            cls = square(offset)
            far = [
                uh_at(uh_ref, i, c, a, h) if offset[i] != 0 else None for i in range(3)
            ]
            reach = combined(far, offset)
            along = combined(
                [far[i] - own[i] if offset[i] != 0 else None for i in range(3)], offset
            )
            rows = pl.ds((a + 2) * SH + h, 8, stride=SH)
            far_pressure = ph_ref[c + 3, rows, :]
            far_shear = ph_ref[7 + c + 3, rows, :]
            value = far_pressure + (far_shear * along + shear * reach) * (1.0 / cls)
            column[c] = jnp.where(
                bit(word, number), value * (1.0 / math.sqrt(cls)), 0.0
            )
            if position + 1 == len(bonds) or bonds[position + 1][1][:2] != (a, b):
                force = fold(force, column, a, b)
                column = {}
        step = step_ref[y]
        for i in range(3):
            rows = pl.ds(i * 64 + y, 8, stride=8)
            velocity = v_ref[rows, :] + force[i] * step
            new_v_ref[rows, :] = velocity
            new_u_ref[rows, :] = u_ref[rows, :] + time_step * velocity


def call(body, outs, args, unplaced=(), scratch=(), flops=1000):
    vmem = pl.BlockSpec(memory_space=pltpu.VMEM)
    unmoved = pl.BlockSpec(memory_space=pltpu.HBM)
    return pl.pallas_call(
        body,
        out_shape=[jax.ShapeDtypeStruct(shape, dtype) for shape, dtype in outs],
        in_specs=[unmoved if position in unplaced else vmem for position in range(len(args))],
        out_specs=[vmem for _ in outs],
        scratch_shapes=scratch,
        cost_estimate=pl.CostEstimate(flops=flops, bytes_accessed=100000, transcendentals=0),
        compiler_params=pltpu.CompilerParams(vmem_limit_bytes=16 * 1024 * 1024),
    )(
        *[
            pltpu.with_memory_space_constraint(arg, pltpu.HBM) if position in unplaced else arg
            for position, arg in enumerate(args)
        ]
    )


def along_y(down, up):
    size = lax.axis_size("gy")
    upward = [(i, i + 1) for i in range(size - 1)]
    downward = [(i + 1, i) for i in range(size - 1)]
    below = lax.ppermute(up, "gy", upward)
    above = lax.ppermute(down, "gy", downward)
    return below, above


def on_device(displacement, velocity, region, bond_words, moduli):
    copy = pltpu.SemaphoreType.DMA(())
    odd, even, u, words, region = call(
        slabs_x,
        [((SLAB, 8, LANES), F32)] * 2
        + [(x.shape, x.dtype) for x in (displacement, bond_words, region)],
        (displacement, bond_words, region),
        unplaced=(0, 1, 2),
        scratch=[copy, copy, copy],
    )
    size = lax.axis_size("gx")
    odd = lax.ppermute(odd, "gx", [(i, ((i - 1) ^ 1) + 1) for i in range(1, size - 1)])
    even = lax.ppermute(even, "gx", [(i, i ^ 1) for i in range(size)])
    even = even.reshape(SLAB * 8, LANES)
    odd = odd.reshape(SLAB * 8, LANES)
    u = u.reshape(192, LANES)
    down, up = call(slabs_y, [((162, LANES), F32)] * 2, (u, even, odd))
    below, above = along_y(down, up)
    ux, wx, part, step = call(
        inner_dilatation,
        [((21, 24 * SU, LANES), F32), ((12, 24 * SW, LANES), jnp.int32), ((48, 8, LANES), F32), ((8, 8, LANES), F32)],
        (u, words.reshape(704, LANES), region.reshape(64, LANES), moduli, even, odd),
        unplaced=(3,),
        scratch=[pltpu.SMEM(moduli.shape, F32), copy],
        flops=40_000_000,
    )
    uh, ps, down, up = call(
        outer_dilatation,
        [
            ((21, 20 * SH, LANES), F32),
            ((2, 16 * SP, LANES), F32),
            ((72, LANES), F32),
            ((72, LANES), F32),
        ],
        (below, above, wx, part),
        flops=4_000_000,
    )
    below, above = along_y(down, up)
    (force,) = call(
        inner_force,
        [((24, 8, LANES), F32)],
        (ux, wx, ps),
        scratch=[pltpu.VMEM((14, 16 * SU, LANES), F32)],
        flops=40_000_000,
    )
    new_u, new_v = call(
        outer_force,
        [((192, LANES), F32)] * 2,
        (below, above, ux, uh, wx, ps, force, u, velocity.reshape(192, LANES), step),
        scratch=[pltpu.VMEM((14, 12 * SH, LANES), F32)],
        flops=4_000_000,
    )
    return new_u.reshape(displacement.shape), new_v.reshape(velocity.shape)


def solution(mesh):
    placed = (
        P(None, "gx", "gy", None),
        P(None, "gx", "gy", None),
        P("gx", "gy", None),
        P(None, "gx", "gy", None),
        P(),
    )
    return jax.shard_map(
        on_device,
        mesh=mesh,
        in_specs=placed,
        out_specs=(P(None, "gx", "gy", None), P(None, "gx", "gy", None)),
        check_vma=False,
    )
```

```python
import math

import jax
import jax.numpy as jnp
from jax import lax
from jax.experimental import pallas as pl
from jax.experimental.pallas import tpu as pltpu
from jax.sharding import PartitionSpec as P


HORIZON = 3
time_step = 0.3
bits_per_word = 12
F32 = jnp.float32
LANES = 128

OFFSETS = [
    (a, b, c)
    for a in range(-HORIZON, HORIZON + 1)
    for b in range(-HORIZON, HORIZON + 1)
    for c in range(-HORIZON, HORIZON + 1)
    if 0 < a * a + b * b + c * c <= HORIZON * HORIZON
]
CLASSES = sorted({a * a + b * b + c * c for a, b, c in OFFSETS})
NUMBERS = {offset: number for number, offset in enumerate(OFFSETS)}
WORDS = (len(OFFSETS) + bits_per_word - 1) // bits_per_word


def square(offset):
    return offset[0] * offset[0] + offset[1] * offset[1] + offset[2] * offset[2]


SU = 14
SW = 9
SH = 7
SF = 9
BLOCKS = (-4, 4)
U_TILE = 44
R_TILE = 62
SLAB = 65
FIELDS = 162
EDGE_ROWS = (0, 1, 2, 5, 6, 7)


def rolled(value, shift):
    return value if shift == 0 else pltpu.roll(value, (-shift) % LANES, 1)


def u_at(ref, component, shift, x, y):
    return ref[component * 7 + shift + 3, pl.ds((x + 8) * SU + y + 3, 8, stride=SU), :]


def word_at(ref, k, x, y):
    return ref[k, pl.ds((x + 8) * SW + y, 8, stride=SW), :]


def uh_at(ref, component, shift, x, h):
    return ref[component * 7 + shift + 3, pl.ds((x + 6) * SH + h, 8, stride=SH), :]


def scaled(value, factor):
    if factor == 1:
        return value
    if factor == -1:
        return -value
    return value * float(factor)


def combined(values, offset):
    total = None
    for value, factor in zip(values, offset):
        if factor == 0:
            continue
        if total is None:
            total = scaled(value, factor)
        elif factor == 1:
            total = total + value
        elif factor == -1:
            total = total - value
        else:
            total = total + value * float(factor)
    return total


def bit(word, number):
    return (word & (1 << (number % bits_per_word))) != 0


def add_to(store, key, value):
    store[key] = value if store.get(key) is None else store[key] + value


def by_class(store):
    total = None
    for cls, value in store.items():
        term = value * (1.0 / math.sqrt(cls))
        total = term if total is None else total + term
    return total


def chosen(region, moduli_ref, row):
    value = jnp.where(region == 1, moduli_ref[row, 1], moduli_ref[row, 0])
    value = jnp.where(region == 2, moduli_ref[row, 2], value)
    return jnp.where(region == 3, moduli_ref[row, 3], value)


def px_at(ref, shift, x, y):
    return ref[shift + 3, pl.ds((x + 4) * SU + y + 3, 8, stride=SU), :]


def field_at(ref, field, x, y):
    return ref[field, pl.ds((x + 4) * SF + y, 8, stride=SF), :]


def crossing(y):
    found = []
    for number, offset in enumerate(OFFSETS):
        target = y + offset[1]
        if target < 0:
            found.append((number, offset, target + 3))
        elif target > 7:
            found.append((number, offset, target - 8 + 3))
    return found


def slabs_x(
    u_hbm, w_hbm, r_hbm, odd_ref, even_ref, u_ref, w_ref, r_ref, u_sem, w_sem, r_sem
):
    parity = lax.axis_index("gx") % 2
    copies = [
        pltpu.make_async_copy(w_hbm, w_ref, w_sem),
        pltpu.make_async_copy(u_hbm, u_ref, u_sem),
        pltpu.make_async_copy(r_hbm, r_ref, r_sem),
    ]
    for copy in copies:
        copy.start()
    for copy in copies:
        copy.wait()
    for ref, right in ((even_ref, 1 - parity), (odd_ref, parity)):
        for k in range(WORDS):
            for d in range(4):
                ref[k * 4 + d] = w_ref[k, right * 4 + d].astype(F32)
        for c in range(3):
            for d in range(6):
                ref[U_TILE + c * 6 + d] = u_ref[c, right * 2 + d]
        for d in range(3):
            ref[R_TILE + d] = r_ref[right * 5 + d].astype(F32)


def halves(even_ref, odd_ref, parity, tile_left, tile_right, y):
    def pick(tile, left):
        rows = pl.ds(tile * 8 + y, 8, stride=8)
        even, odd = (even_ref[rows, :], odd_ref[rows, :])
        return jnp.where(parity == 0, odd, even) if left else jnp.where(parity == 0, even, odd)

    return pick(tile_left, True), pick(tile_right, False)


def inner_sum(ux_ref, wx_ref, x0, y):
    own = [u_at(ux_ref, c, 0, x0, y) for c in range(3)]
    sums = {}
    word = None
    for number, offset in enumerate(OFFSETS):
        if number % bits_per_word == 0:
            word = word_at(wx_ref, number // bits_per_word, x0, y)
        difference = [
            u_at(ux_ref, c, offset[2], x0 + offset[0], y + offset[1]) - own[c]
            if offset[c] != 0
            else None
            for c in range(3)
        ]
        along = combined(difference, offset)
        add_to(sums, square(offset), jnp.where(bit(word, number), along, 0.0))
    return by_class(sums)


def ratios(wx_ref, moduli_ref, x0, y):
    counts = {}
    for k in range(WORDS):
        word = word_at(wx_ref, k, x0, y)
        group = OFFSETS[k * bits_per_word : (k + 1) * bits_per_word]
        for cls in CLASSES:
            held = sum(1 << i for i, offset in enumerate(group) if square(offset) == cls)
            if held:
                add_to(counts, cls, lax.population_count(word & held))
    volume = None
    for cls in CLASSES:
        term = counts[cls].astype(F32) * math.sqrt(cls)
        volume = term if volume is None else volume + term
    inverse = 1.0 / jnp.where(volume > 0.0, volume, 1.0)
    region = word_at(wx_ref, WORDS, x0, y)
    bulk = chosen(region, moduli_ref, 0)
    shear = chosen(region, moduli_ref, 1)
    return (3.0 * inverse) * ((3.0 * bulk - 5.0 * shear) * inverse), 15.0 * shear * inverse


def slabs_y(
    u_ref,
    w_ref,
    r_ref,
    moduli_hbm,
    even_ref,
    odd_ref,
    ux_ref,
    wx_ref,
    field_ref,
    down_ref,
    up_ref,
    moduli_ref,
    moduli_sem,
):
    fetch = pltpu.make_async_copy(moduli_hbm, moduli_ref, moduli_sem)
    fetch.start()
    parity = lax.axis_index("gx") % 2
    zero = jnp.zeros((8, LANES), F32)
    for y in (-3, -2, -1, 8, 9, 10):
        for lead in range(21):
            for x in (-8, 0, 8):
                ux_ref[lead, pl.ds((x + 8) * SU + y + 3, 8, stride=SU), :] = zero
    for y in range(8):
        for c in range(3):
            tile = U_TILE + c * 6
            left, right = halves(even_ref, odd_ref, parity, tile - 2, tile, y)
            own = u_ref[pl.ds(c * 64 + y, 8, stride=8), :]
            for x, value in ((-8, left), (8, right), (0, own)):
                for shift in range(-3, 4):
                    ux_ref[
                        c * 7 + shift + 3, pl.ds((x + 8) * SU + y + 3, 8, stride=SU), :
                    ] = rolled(value, shift)
        for k in range(WORDS + 1):
            if k < WORDS:
                left, right = halves(even_ref, odd_ref, parity, k * 4, k * 4, y)
                own = w_ref[pl.ds(k * 64 + y, 8, stride=8), :]
                places = (-4, 8)
            else:
                left, right = halves(even_ref, odd_ref, parity, R_TILE - 5, R_TILE - 5, y)
                own = r_ref[pl.ds(y, 8, stride=8), :]
                places = (-8, 3)
            for x, value in (
                (places[0], left.astype(jnp.int32)),
                (places[1], right.astype(jnp.int32)),
                (0, own),
            ):
                wx_ref[k, pl.ds((x + 8) * SW + y, 8, stride=SW), :] = value

    def row(index, carry):
        y = index + jnp.where(index < 3, 0, 2)
        for x0 in BLOCKS:
            field_ref[0, pl.ds((x0 + 4) * SF + y, 8, stride=SF), :] = inner_sum(
                ux_ref, wx_ref, x0, y
            )
        return carry

    lax.fori_loop(0, 6, row, 0)
    fetch.wait()
    for y in EDGE_ROWS:
        for x0 in BLOCKS:
            rows = pl.ds((x0 + 4) * SF + y, 8, stride=SF)
            field_ref[1, rows, :], field_ref[2, rows, :] = ratios(wx_ref, moduli_ref, x0, y)
    for ref, first in ((down_ref, 0), (up_ref, 5)):
        for i in range(3):
            for d in range(3):
                y = first + d
                j = i * 3 + d
                for x in (-5, 3, 5):
                    ref[pl.ds((x + 5) * 9 + j, 8, stride=9), :] = u_at(ux_ref, i, 0, x, y)
                for x in (-2, 2):
                    ref[pl.ds(FIELDS + (x + 2) * 9 + j, 8, stride=9), :] = field_at(
                        field_ref, i, x, y
                    )


def fold(force, column, a, b):
    force = list(force)
    total = None
    for value in column.values():
        total = value if total is None else total + value
    for i, factor in ((0, a), (1, b)):
        if factor != 0:
            term = scaled(total, factor)
            force[i] = term if force[i] is None else force[i] + term
    for c, value in column.items():
        if c > 0:
            term = scaled(value - column[-c], c)
            force[2] = term if force[2] is None else force[2] + term
    return force


def inner_force(
    ux_ref,
    wx_ref,
    field_ref,
    moduli_hbm,
    middle_ref,
    part_ref,
    sum_ref,
    step_ref,
    sx_ref,
    moduli_ref,
    moduli_sem,
):
    fetch = pltpu.make_async_copy(moduli_hbm, moduli_ref, moduli_sem)
    fetch.start()
    zero = jnp.zeros((8, LANES), F32)
    for x in BLOCKS:
        for y in (-3, -2, -1, 8, 9, 10):
            for lead in range(7):
                sx_ref[lead, pl.ds((x + 4) * SU + y + 3, 8, stride=SU), :] = zero
    fetch.wait()
    for y in range(8):
        step_ref[y] = time_step / chosen(word_at(wx_ref, WORDS, 0, y), moduli_ref, 2)
        for index, x in enumerate(BLOCKS):
            if y in EDGE_ROWS:
                shear = field_at(field_ref, 2, x, y)
            else:
                place = (index * 2 + y - 3) * 3
                middle_ref[place] = inner_sum(ux_ref, wx_ref, x, y)
                middle_ref[place + 1], shear = ratios(wx_ref, moduli_ref, x, y)
                middle_ref[place + 2] = shear
            for shift in range(-3, 4):
                sx_ref[
                    shift + 3, pl.ds((x + 4) * SU + y + 3, 8, stride=SU), :
                ] = rolled(shear, shift)

    def row(y, carry):
        own = [u_at(ux_ref, c, 0, 0, y) for c in range(3)]
        shear = px_at(sx_ref, 0, 0, y)
        force = [None, None, None]
        balance = [None, None, None]
        word = None
        column = {}
        count = {}
        for number, offset in enumerate(OFFSETS):
            if number % bits_per_word == 0:
                word = word_at(wx_ref, number // bits_per_word, 0, y)
            a, b, c = offset
            difference = [
                u_at(ux_ref, i, c, a, y + b) - own[i] if offset[i] != 0 else None
                for i in range(3)
            ]
            cls = square(offset)
            value = (shear + px_at(sx_ref, c, a, y + b)) * combined(difference, offset)
            held = bit(word, number)
            column[c] = jnp.where(held, value * (1.0 / (cls * math.sqrt(cls))), 0.0)
            count[c] = jnp.where(held, F32(1.0 / math.sqrt(cls)), F32(0.0))
            if number + 1 == len(OFFSETS) or OFFSETS[number + 1][:2] != (a, b):
                force = fold(force, column, a, b)
                balance = fold(balance, count, a, b)
                column = {}
                count = {}
        for i in range(3):
            part_ref[i * 8 + y] = force[i]
            sum_ref[i * 8 + y] = balance[i]
        return carry

    lax.fori_loop(0, 8, row, 0)


def halo_y(h):
    return h - 3 if h < 3 else h + 5


def outer_force(
    below_ref,
    above_ref,
    ux_ref,
    wx_ref,
    field_ref,
    middle_ref,
    part_ref,
    sum_ref,
    step_ref,
    u_ref,
    v_ref,
    new_u_ref,
    new_v_ref,
    uh_ref,
    hd_ref,
    sh_ref,
    px_ref,
    force_ref,
):
    halo = (below_ref, above_ref)
    zero = jnp.zeros((8, LANES), F32)
    for h in range(6):
        for i in range(3):
            for x in (-5, 3, 5):
                value = halo[h // 3][pl.ds((x + 5) * 9 + i * 3 + h % 3, 8, stride=9), :]
                for shift in range(-3, 4):
                    uh_ref[
                        i * 7 + shift + 3, pl.ds((x + 6) * SH + h, 8, stride=SH), :
                    ] = rolled(value, shift)
        for x in (-6, 2, 6):
            hd_ref[pl.ds((x + 6) * SH + h, 8, stride=SH), :] = zero

    for index, x0 in enumerate(BLOCKS):
        rest = {}
        for h in range(6):
            for a in range(-2, 3):
                spread = None
                for c in range(-2, 3):
                    gathered = None
                    for y in range(8):
                        offset = (a, halo_y(h) - y, c)
                        if offset not in NUMBERS:
                            continue
                        number = NUMBERS[offset]
                        factor = 1.0 / math.sqrt(square(offset))
                        held = bit(word_at(wx_ref, number // bits_per_word, x0, y), number)
                        far = [
                            uh_at(uh_ref, i, c, x0 + a, h) if offset[i] != 0 else None
                            for i in range(3)
                        ]
                        own = [
                            u_at(ux_ref, i, 0, x0, y) if offset[i] != 0 else None
                            for i in range(3)
                        ]
                        add_to(
                            rest, y, jnp.where(held, combined(far, offset) * factor, 0.0)
                        )
                        term = jnp.where(held, combined(own, offset) * factor, 0.0)
                        gathered = term if gathered is None else gathered + term
                    if gathered is not None:
                        value = rolled(gathered, -c)
                        spread = value if spread is None else spread + value
                if spread is not None:
                    rows = pl.ds((x0 + a + 6) * SH + h, 8, stride=SH)
                    hd_ref[rows, :] = hd_ref[rows, :] - spread
        for y in range(8):
            if y in EDGE_ROWS:
                total = field_at(field_ref, 0, x0, y) + rest[y]
                pressure = total * field_at(field_ref, 1, x0, y)
            else:
                place = (index * 2 + y - 3) * 3
                pressure = middle_ref[place] * middle_ref[place + 1]
            for shift in range(-3, 4):
                px_ref[
                    shift + 3, pl.ds((x0 + 4) * SU + y + 3, 8, stride=SU), :
                ] = rolled(pressure, shift)
    for h in range(6):
        for x in (-2, 2):
            part, ratio, shear = [
                halo[h // 3][pl.ds(FIELDS + (x + 2) * 9 + i * 3 + h % 3, 8, stride=9), :]
                for i in range(3)
            ]
            pressure = (part + hd_ref[pl.ds((x + 6) * SH + h, 8, stride=SH), :]) * ratio
            for shift in range(-3, 4):
                px_ref[
                    shift + 3, pl.ds((x + 4) * SU + halo_y(h) + 3, 8, stride=SU), :
                ] = rolled(pressure, shift)
                sh_ref[shift + 3, pl.ds((x + 2) * SH + h, 8, stride=SH), :] = rolled(
                    shear, shift
                )

    def row(y, carry):
        pressure = px_at(px_ref, 0, 0, y)
        force = [part_ref[i * 8 + y] + pressure * sum_ref[i * 8 + y] for i in range(3)]
        word = None
        column = {}
        for number, offset in enumerate(OFFSETS):
            if number % bits_per_word == 0:
                word = word_at(wx_ref, number // bits_per_word, 0, y)
            a, b, c = offset
            column[c] = jnp.where(
                bit(word, number),
                px_at(px_ref, c, a, y + b) * (1.0 / math.sqrt(square(offset))),
                0.0,
            )
            if number + 1 == len(OFFSETS) or OFFSETS[number + 1][:2] != (a, b):
                force = fold(force, column, a, b)
                column = {}
        for i in range(3):
            force_ref[i * 8 + y] = force[i]
        return carry

    lax.fori_loop(0, 8, row, 0)

    for y in range(8):
        force = [force_ref[i * 8 + y] for i in range(3)]
        own = [u_at(ux_ref, c, 0, 0, y) for c in range(3)]
        if y in EDGE_ROWS:
            shear = field_at(field_ref, 2, 0, y)
        column = {}
        bonds = crossing(y)
        for position, (number, offset, h) in enumerate(bonds):
            word = word_at(wx_ref, number // bits_per_word, 0, y)
            a, b, c = offset
            cls = square(offset)
            far = [
                uh_at(uh_ref, i, c, a, h) if offset[i] != 0 else None for i in range(3)
            ]
            reach = combined(far, offset)
            along = combined(
                [far[i] - own[i] if offset[i] != 0 else None for i in range(3)], offset
            )
            far_shear = sh_ref[c + 3, pl.ds((a + 2) * SH + h, 8, stride=SH), :]
            value = (far_shear * along + shear * reach) * (1.0 / (cls * math.sqrt(cls)))
            column[c] = jnp.where(bit(word, number), value, 0.0)
            if position + 1 == len(bonds) or bonds[position + 1][1][:2] != (a, b):
                force = fold(force, column, a, b)
                column = {}
        step = step_ref[y]
        for i in range(3):
            rows = pl.ds(i * 64 + y, 8, stride=8)
            velocity = v_ref[rows, :] + force[i] * step
            new_v_ref[rows, :] = velocity
            new_u_ref[rows, :] = u_ref[rows, :] + time_step * velocity


def call(body, outs, args, unplaced=(), scratch=(), flops=1000):
    vmem = pl.BlockSpec(memory_space=pltpu.VMEM)
    unmoved = pl.BlockSpec(memory_space=pltpu.HBM)
    return pl.pallas_call(
        body,
        out_shape=[jax.ShapeDtypeStruct(shape, dtype) for shape, dtype in outs],
        in_specs=[unmoved if position in unplaced else vmem for position in range(len(args))],
        out_specs=[vmem for _ in outs],
        scratch_shapes=scratch,
        cost_estimate=pl.CostEstimate(flops=flops, bytes_accessed=100000, transcendentals=0),
        compiler_params=pltpu.CompilerParams(vmem_limit_bytes=16 * 1024 * 1024),
    )(
        *[
            pltpu.with_memory_space_constraint(arg, pltpu.HBM) if position in unplaced else arg
            for position, arg in enumerate(args)
        ]
    )


def along_y(down, up):
    size = lax.axis_size("gy")
    upward = [(i, i + 1) for i in range(size - 1)]
    downward = [(i + 1, i) for i in range(size - 1)]
    below = lax.ppermute(up, "gy", upward)
    above = lax.ppermute(down, "gy", downward)
    return below, above


def on_device(displacement, velocity, region, bond_words, moduli):
    copy = pltpu.SemaphoreType.DMA(())
    odd, even, u, words, region = call(
        slabs_x,
        [((SLAB, 8, LANES), F32)] * 2
        + [(x.shape, x.dtype) for x in (displacement, bond_words, region)],
        (displacement, bond_words, region),
        unplaced=(0, 1, 2),
        scratch=[copy, copy, copy],
    )
    size = lax.axis_size("gx")
    odd = lax.ppermute(
        odd, "gx", [(i, ((i - 1) ^ 1) + 1) for i in range(1, size - 1)]
    )
    even = lax.ppermute(even, "gx", [(i, i ^ 1) for i in range(size)])
    even = even.reshape(SLAB * 8, LANES)
    odd = odd.reshape(SLAB * 8, LANES)
    u = u.reshape(192, LANES)
    ux, wx, fields, down, up = call(
        slabs_y,
        [
            ((21, 24 * SU, LANES), F32),
            ((12, 24 * SW, LANES), jnp.int32),
            ((3, 16 * SF, LANES), F32),
            ((FIELDS + 108, LANES), F32),
            ((FIELDS + 108, LANES), F32),
        ],
        (u, words.reshape(704, LANES), region.reshape(64, LANES), moduli, even, odd),
        unplaced=(3,),
        scratch=[pltpu.SMEM(moduli.shape, F32), copy],
        flops=20_000_000,
    )
    below, above = along_y(down, up)
    middle, part, balance, step = call(
        inner_force,
        [
            ((12, 8, LANES), F32),
            ((24, 8, LANES), F32),
            ((24, 8, LANES), F32),
            ((8, 8, LANES), F32),
        ],
        (ux, wx, fields, moduli),
        unplaced=(3,),
        scratch=[
            pltpu.VMEM((7, 16 * SU, LANES), F32),
            pltpu.SMEM(moduli.shape, F32),
            copy,
        ],
        flops=40_000_000,
    )
    new_u, new_v = call(
        outer_force,
        [((192, LANES), F32)] * 2,
        (
            below,
            above,
            ux,
            wx,
            fields,
            middle,
            part,
            balance,
            step,
            u,
            velocity.reshape(192, LANES),
        ),
        scratch=[
            pltpu.VMEM((21, 20 * SH, LANES), F32),
            pltpu.VMEM((20 * SH, LANES), F32),
            pltpu.VMEM((7, 12 * SH, LANES), F32),
            pltpu.VMEM((7, 16 * SU, LANES), F32),
            pltpu.VMEM((24, 8, LANES), F32),
        ],
        flops=10_000_000,
    )
    return new_u.reshape(displacement.shape), new_v.reshape(velocity.shape)


def solution(mesh):
    placed = (
        P(None, "gx", "gy", None),
        P(None, "gx", "gy", None),
        P("gx", "gy", None),
        P(None, "gx", "gy", None),
        P(),
    )
    return jax.shard_map(
        on_device,
        mesh=mesh,
        in_specs=placed,
        out_specs=(P(None, "gx", "gy", None), P(None, "gx", "gy", None)),
        check_vma=False,
    )
```

```python
import math

import jax
import jax.numpy as jnp
from jax import lax
from jax.experimental import pallas as pl
from jax.experimental.pallas import tpu as pltpu
from jax.sharding import PartitionSpec as P


HORIZON = 3
time_step = 0.3
bits_per_word = 12
F32 = jnp.float32
LANES = 128

OFFSETS = [
    (a, b, c)
    for a in range(-HORIZON, HORIZON + 1)
    for b in range(-HORIZON, HORIZON + 1)
    for c in range(-HORIZON, HORIZON + 1)
    if 0 < a * a + b * b + c * c <= HORIZON * HORIZON
]
CLASSES = sorted({a * a + b * b + c * c for a, b, c in OFFSETS})
NUMBERS = {offset: number for number, offset in enumerate(OFFSETS)}
WORDS = (len(OFFSETS) + bits_per_word - 1) // bits_per_word


def square(offset):
    return offset[0] * offset[0] + offset[1] * offset[1] + offset[2] * offset[2]


UX_ROWS = 20 * 28
WX_ROWS = 16 * 18
FX_ROWS = 16 * 18
SU = 14
SH = 7
BLOCKS = (-4, 4)
EXTRA_TILE = 33
U_TILE = 36
R_TILE = 54
SLAB = 57
SLAB_Y = 246
EDGE_ROWS = (0, 1, 2, 5, 6, 7)


def rolled(value, shift):
    return value if shift == 0 else pltpu.roll(value, (-shift) % LANES, 1)


def ux_rows(x, y):
    return pl.ds(((x + 6) * 14 + y + 3) * 2, 8, stride=28)


def ux_column(x, y=0):
    return pl.ds(((x + 6) * 14 + y + 3) * 2, 8, stride=2)


def fx_rows(x, y):
    return pl.ds(((x + 4) * 9 + y) * 2, 8, stride=18)


def fx_column(x):
    return pl.ds((x + 4) * 18, 8, stride=2)


def u_at(ref, component, shift, x, y):
    return ref[component * 7 + shift + 3, ux_rows(x, y), :]


def word_at(ref, k, x, y):
    return ref[k, fx_rows(x, y), :]


def uh_at(ref, component, shift, x, h):
    return ref[component * 5 + shift + 2, pl.ds((x + 6) * SH + h, 8, stride=SH), :]


def slab_u(component, depth, x):
    if depth < 2:
        return pl.ds((x + 5) * 6 + component * 2 + depth, 8, stride=6)
    return pl.ds(108 + (x + 3) * 3 + component, 8, stride=3)


def slab_field(field, depth, x):
    if depth < 2:
        return pl.ds(150 + (x + 2) * 6 + field * 2 + depth, 8, stride=6)
    return pl.ds(222 + x * 3 + field, 8, stride=3)


def slab_places(depth):
    return ((-5, 3, 5), (-2, 2)) if depth < 2 else ((-3, 3), (0,))


def scaled(value, factor):
    if factor == 1:
        return value
    if factor == -1:
        return -value
    return value * float(factor)


def combined(values, offset):
    total = None
    for value, factor in zip(values, offset):
        if factor == 0:
            continue
        if total is None:
            total = scaled(value, factor)
        elif factor == 1:
            total = total + value
        elif factor == -1:
            total = total - value
        else:
            total = total + value * float(factor)
    return total


def bit(word, number):
    return (word & (1 << (number % bits_per_word))) != 0


def add_to(store, key, value):
    store[key] = value if store.get(key) is None else store[key] + value


def by_class(store):
    total = None
    for cls, value in store.items():
        term = value * (1.0 / math.sqrt(cls))
        total = term if total is None else total + term
    return total


def chosen(region, moduli_ref, row):
    value = jnp.where(region == 1, moduli_ref[row, 1], moduli_ref[row, 0])
    value = jnp.where(region == 2, moduli_ref[row, 2], value)
    return jnp.where(region == 3, moduli_ref[row, 3], value)


def px_at(ref, shift, x, y):
    return ref[shift + 3, pl.ds((x + 4) * SU + y + 3, 8, stride=SU), :]


def field_at(ref, field, x, y):
    return ref[field, fx_rows(x, y), :]


def crossing(y):
    found = []
    for number, offset in enumerate(OFFSETS):
        target = y + offset[1]
        if target < 0:
            found.append((number, offset, target + 3))
        elif target > 7:
            found.append((number, offset, target - 8 + 3))
    return found


def slabs_x(
    u_hbm, w_hbm, r_hbm, odd_ref, even_ref, u_ref, w_ref, r_ref, u_sem, w_sem, r_sem
):
    parity = lax.axis_index("gx") % 2
    copies = [
        pltpu.make_async_copy(w_hbm, w_ref, w_sem),
        pltpu.make_async_copy(u_hbm, u_ref, u_sem),
        pltpu.make_async_copy(r_hbm, r_ref, r_sem),
    ]
    for copy in copies:
        copy.start()
    for copy in copies:
        copy.wait()
    for ref, right in ((even_ref, 1 - parity), (odd_ref, parity)):
        for k in range(WORDS):
            for d in range(3):
                ref[k * 3 + d] = w_ref[k, right * 5 + d].astype(F32)
        for d in range(3):
            ref[EXTRA_TILE + d] = w_ref[right * 8 + d, right + 3].astype(F32)
        for c in range(3):
            for d in range(6):
                ref[U_TILE + c * 6 + d] = u_ref[c, right * 2 + d]
        for d in range(3):
            ref[R_TILE + d] = r_ref[right * 5 + d].astype(F32)


def column_sum(ux_ref, words, x, inside):
    own = [ux_ref[i * 7 + 3, ux_column(x), :] for i in range(3)]
    sums = {}
    loaded = None
    for number, offset in enumerate(OFFSETS):
        if not inside(x + offset[0]):
            continue
        if loaded != number // bits_per_word:
            loaded = number // bits_per_word
            word = words(loaded)
        difference = [
            ux_ref[i * 7 + offset[2] + 3, ux_column(x + offset[0], offset[1]), :] - own[i]
            if offset[i] != 0
            else None
            for i in range(3)
        ]
        along = combined(difference, offset)
        add_to(sums, square(offset), jnp.where(bit(word, number), along, 0.0))
    return by_class(sums)


def ratios(words, region, moduli_ref):
    counts = {}
    for k in range(WORDS):
        word = words(k)
        group = OFFSETS[k * bits_per_word : (k + 1) * bits_per_word]
        for cls in CLASSES:
            held = sum(1 << i for i, offset in enumerate(group) if square(offset) == cls)
            if held:
                add_to(counts, cls, lax.population_count(word & held))
    volume = None
    for cls in CLASSES:
        term = counts[cls].astype(F32) * math.sqrt(cls)
        volume = term if volume is None else volume + term
    inverse = 1.0 / jnp.where(volume > 0.0, volume, 1.0)
    bulk = chosen(region, moduli_ref, 0)
    shear = chosen(region, moduli_ref, 1)
    return (3.0 * inverse) * ((3.0 * bulk - 5.0 * shear) * inverse), 15.0 * shear * inverse


def spread_column(ux_ref, component, x, value):
    for shift in range(-3, 4):
        ux_ref[component * 7 + shift + 3, ux_column(x), :] = rolled(value, shift)


def own_part(u_ref, w_ref, r_ref, moduli_hbm, ux_ref, own_ref, moduli_ref, moduli_sem):
    fetch = pltpu.make_async_copy(moduli_hbm, moduli_ref, moduli_sem)
    fetch.start()
    zero = jnp.zeros((8, LANES), F32)
    for i in range(3):
        for x in range(8):
            spread_column(ux_ref, i, x, u_ref[pl.ds(i * 64 + x * 8, 8), :])
        for shift in range(-2, 3):
            for y in (-3, -2, -1, 8, 9, 10):
                for x in (-6, 2, 6):
                    ux_ref[i * 7 + shift + 3, ux_rows(x, y), :] = zero
    for x in range(8):
        own_ref[x] = column_sum(
            ux_ref,
            lambda k, x=x: w_ref[pl.ds(k * 64 + x * 8, 8), :],
            x,
            lambda far: 0 <= far < 8,
        )
    fetch.wait()
    for x in range(8):
        own_ref[8 + x], own_ref[16 + x] = ratios(
            lambda k, x=x: w_ref[pl.ds(k * 64 + x * 8, 8), :],
            r_ref[pl.ds(x * 8, 8), :],
            moduli_ref,
        )


def halo_reader(even_ref, odd_ref):
    parity = lax.axis_index("gx") % 2

    def tile(index, left):
        rows = pl.ds(index * 8, 8)
        even, odd = (even_ref[rows, :], odd_ref[rows, :])
        return jnp.where(parity == 0, odd, even) if left else jnp.where(parity == 0, even, odd)

    def word(k, x):
        d = x + 3 if x < 0 else x - 8
        return tile(k * 3 + d, x < 0).astype(jnp.int32)

    def region(x):
        d = x + 3 if x < 0 else x - 8
        return tile(R_TILE + d, x < 0).astype(jnp.int32)

    return tile, word, region


def slabs_y(
    u_ref,
    w_ref,
    own_ref,
    moduli_hbm,
    even_ref,
    odd_ref,
    ux_in_ref,
    ux_ref,
    field_ref,
    down_ref,
    up_ref,
    moduli_ref,
    moduli_sem,
):
    fetch = pltpu.make_async_copy(moduli_hbm, moduli_ref, moduli_sem)
    fetch.start()
    tile, halo_word, halo_region = halo_reader(even_ref, odd_ref)
    for i in range(3):
        for d in range(6):
            spread_column(ux_ref, i, d - 6, tile(U_TILE + i * 6 + d, True))
            spread_column(ux_ref, i, d + 8, tile(U_TILE + i * 6 + d, False))
    for x in range(8):
        value = own_ref[x]
        if x < 3 or x > 4:
            value = value + column_sum(
                ux_ref,
                lambda k, x=x: w_ref[pl.ds(k * 64 + x * 8, 8), :],
                x,
                lambda far: far < 0 or far > 7,
            )
        field_ref[0, fx_column(x), :] = value
        field_ref[1, fx_column(x), :] = own_ref[8 + x]
        field_ref[2, fx_column(x), :] = own_ref[16 + x]
    for x in (-2, -1, 8, 9):
        field_ref[0, fx_column(x), :] = column_sum(
            ux_ref, lambda k, x=x: halo_word(k, x), x, lambda far: True
        )
    fetch.wait()
    for x in (-2, -1, 8, 9):
        field_ref[1, fx_column(x), :], field_ref[2, fx_column(x), :] = ratios(
            lambda k, x=x: halo_word(k, x), halo_region(x), moduli_ref
        )
    for ref, first, step in ((down_ref, 0, 1), (up_ref, 7, -1)):
        for i in range(3):
            for depth in range(3):
                y = first + step * depth
                places, field_places = slab_places(depth)
                for x in places:
                    ref[slab_u(i, depth, x), :] = u_at(ux_ref, i, 0, x, y)
                for x in field_places:
                    ref[slab_field(i, depth, x), :] = field_at(field_ref, i, x, y)


def fold(force, column, a, b):
    force = list(force)
    total = None
    for value in column.values():
        total = value if total is None else total + value
    for i, factor in ((0, a), (1, b)):
        if factor != 0:
            term = scaled(total, factor)
            force[i] = term if force[i] is None else force[i] + term
    for c, value in column.items():
        if c > 0:
            term = scaled(value - column[-c], c)
            force[2] = term if force[2] is None else force[2] + term
    return force


def inner_force(
    ux_ref,
    w_ref,
    r_ref,
    moduli_hbm,
    even_ref,
    odd_ref,
    field_in_ref,
    field_ref,
    wx_ref,
    part_ref,
    sum_ref,
    step_ref,
    sx_ref,
    moduli_ref,
    moduli_sem,
):
    fetch = pltpu.make_async_copy(moduli_hbm, moduli_ref, moduli_sem)
    fetch.start()
    tile, halo_word, halo_region = halo_reader(even_ref, odd_ref)
    for k in range(WORDS):
        for x in range(8):
            wx_ref[k, fx_column(x), :] = w_ref[pl.ds(k * 64 + x * 8, 8), :]
        for x in (-3, -2, -1, 8, 9, 10):
            wx_ref[k, fx_column(x), :] = halo_word(k, x)
    for d in range(3):
        wx_ref[8 + d, fx_column(-4), :] = tile(EXTRA_TILE + d, True).astype(jnp.int32)
        wx_ref[d, fx_column(11), :] = tile(EXTRA_TILE + d, False).astype(jnp.int32)
    zero = jnp.zeros((8, LANES), F32)
    for x in BLOCKS:
        for y in (-3, -2, -1, 8, 9, 10):
            for lead in range(1, 6):
                sx_ref[lead, pl.ds((x + 4) * SU + y + 3, 8, stride=SU), :] = zero
    for x in (-3, 10):
        field_ref[0, fx_column(x), :] = column_sum(
            ux_ref, lambda k, x=x: halo_word(k, x), x, lambda far: True
        )
    fetch.wait()
    for x in (-3, 10):
        field_ref[1, fx_column(x), :], field_ref[2, fx_column(x), :] = ratios(
            lambda k, x=x: halo_word(k, x), halo_region(x), moduli_ref
        )
    for y in range(8):
        step_ref[y] = time_step / chosen(r_ref[pl.ds(y, 8, stride=8), :], moduli_ref, 2)
        for x in BLOCKS:
            shear = field_at(field_ref, 2, x, y)
            for shift in range(-3, 4):
                sx_ref[
                    shift + 3, pl.ds((x + 4) * SU + y + 3, 8, stride=SU), :
                ] = rolled(shear, shift)

    def row(y, carry):
        own = [u_at(ux_ref, c, 0, 0, y) for c in range(3)]
        shear = px_at(sx_ref, 0, 0, y)
        force = [None, None, None]
        balance = [None, None, None]
        word = None
        column = {}
        count = {}
        for number, offset in enumerate(OFFSETS):
            if number % bits_per_word == 0:
                word = word_at(wx_ref, number // bits_per_word, 0, y)
            a, b, c = offset
            difference = [
                u_at(ux_ref, i, c, a, y + b) - own[i] if offset[i] != 0 else None
                for i in range(3)
            ]
            cls = square(offset)
            value = (shear + px_at(sx_ref, c, a, y + b)) * combined(difference, offset)
            held = bit(word, number)
            column[c] = jnp.where(held, value * (1.0 / (cls * math.sqrt(cls))), 0.0)
            count[c] = jnp.where(held, F32(1.0 / math.sqrt(cls)), F32(0.0))
            if number + 1 == len(OFFSETS) or OFFSETS[number + 1][:2] != (a, b):
                force = fold(force, column, a, b)
                balance = fold(balance, count, a, b)
                column = {}
                count = {}
        for i in range(3):
            part_ref[i * 8 + y] = force[i]
            sum_ref[i * 8 + y] = balance[i]
        return carry

    lax.fori_loop(0, 8, row, 0)


def halo_y(h):
    return h - 3 if h < 3 else h + 5


def outer_force(
    below_ref,
    above_ref,
    ux_ref,
    wx_ref,
    field_ref,
    part_ref,
    sum_ref,
    step_ref,
    u_ref,
    v_ref,
    new_u_ref,
    new_v_ref,
    uh_ref,
    hd_ref,
    sh_ref,
    px_ref,
    force_ref,
):
    zero = jnp.zeros((8, LANES), F32)
    halo = [(below_ref, depth, 2 - depth) for depth in range(3)]
    halo += [(above_ref, depth, 3 + depth) for depth in range(3)]
    for ref, depth, h in halo:
        for i in range(3):
            for x in slab_places(depth)[0]:
                value = ref[slab_u(i, depth, x), :]
                for shift in range(-2, 3) if depth < 2 else (0,):
                    uh_ref[
                        i * 5 + shift + 2, pl.ds((x + 6) * SH + h, 8, stride=SH), :
                    ] = rolled(value, shift)
        for x in (-6, 2, 6):
            hd_ref[pl.ds((x + 6) * SH + h, 8, stride=SH), :] = zero

    for x0 in BLOCKS:
        rest = {}
        for h in range(6):
            for a in range(-2, 3):
                spread = None
                for c in range(-2, 3):
                    gathered = None
                    for y in range(8):
                        offset = (a, halo_y(h) - y, c)
                        if offset not in NUMBERS:
                            continue
                        number = NUMBERS[offset]
                        factor = 1.0 / math.sqrt(square(offset))
                        held = bit(word_at(wx_ref, number // bits_per_word, x0, y), number)
                        far = [
                            uh_at(uh_ref, i, c, x0 + a, h) if offset[i] != 0 else None
                            for i in range(3)
                        ]
                        own = [
                            u_at(ux_ref, i, 0, x0, y) if offset[i] != 0 else None
                            for i in range(3)
                        ]
                        add_to(
                            rest, y, jnp.where(held, combined(far, offset) * factor, 0.0)
                        )
                        term = jnp.where(held, combined(own, offset) * factor, 0.0)
                        gathered = term if gathered is None else gathered + term
                    if gathered is not None:
                        value = rolled(gathered, -c)
                        spread = value if spread is None else spread + value
                if spread is not None:
                    rows = pl.ds((x0 + a + 6) * SH + h, 8, stride=SH)
                    hd_ref[rows, :] = hd_ref[rows, :] - spread
        for y in range(8):
            total = field_at(field_ref, 0, x0, y)
            if y in EDGE_ROWS:
                total = total + rest[y]
            pressure = total * field_at(field_ref, 1, x0, y)
            for shift in range(-3, 4):
                px_ref[
                    shift + 3, pl.ds((x0 + 4) * SU + y + 3, 8, stride=SU), :
                ] = rolled(pressure, shift)
    for ref, depth, h in halo:
        for x in slab_places(depth)[1]:
            part, ratio, shear = [ref[slab_field(i, depth, x), :] for i in range(3)]
            pressure = (part + hd_ref[pl.ds((x + 6) * SH + h, 8, stride=SH), :]) * ratio
            for shift in range(-2, 3) if depth < 2 else (0,):
                px_ref[
                    shift + 3, pl.ds((x + 4) * SU + halo_y(h) + 3, 8, stride=SU), :
                ] = rolled(pressure, shift)
                sh_ref[shift + 2, pl.ds((x + 2) * SH + h, 8, stride=SH), :] = rolled(
                    shear, shift
                )

    def row(y, carry):
        pressure = px_at(px_ref, 0, 0, y)
        force = [part_ref[i * 8 + y] + pressure * sum_ref[i * 8 + y] for i in range(3)]
        word = None
        column = {}
        for number, offset in enumerate(OFFSETS):
            if number % bits_per_word == 0:
                word = word_at(wx_ref, number // bits_per_word, 0, y)
            a, b, c = offset
            column[c] = jnp.where(
                bit(word, number),
                px_at(px_ref, c, a, y + b) * (1.0 / math.sqrt(square(offset))),
                0.0,
            )
            if number + 1 == len(OFFSETS) or OFFSETS[number + 1][:2] != (a, b):
                force = fold(force, column, a, b)
                column = {}
        for i in range(3):
            force_ref[i * 8 + y] = force[i]
        return carry

    lax.fori_loop(0, 8, row, 0)

    for y in range(8):
        force = [force_ref[i * 8 + y] for i in range(3)]
        own = [u_at(ux_ref, c, 0, 0, y) for c in range(3)]
        if y in EDGE_ROWS:
            shear = field_at(field_ref, 2, 0, y)
        column = {}
        bonds = crossing(y)
        for position, (number, offset, h) in enumerate(bonds):
            word = word_at(wx_ref, number // bits_per_word, 0, y)
            a, b, c = offset
            cls = square(offset)
            far = [
                uh_at(uh_ref, i, c, a, h) if offset[i] != 0 else None for i in range(3)
            ]
            reach = combined(far, offset)
            along = combined(
                [far[i] - own[i] if offset[i] != 0 else None for i in range(3)], offset
            )
            far_shear = sh_ref[c + 2, pl.ds((a + 2) * SH + h, 8, stride=SH), :]
            value = (far_shear * along + shear * reach) * (1.0 / (cls * math.sqrt(cls)))
            column[c] = jnp.where(bit(word, number), value, 0.0)
            if position + 1 == len(bonds) or bonds[position + 1][1][:2] != (a, b):
                force = fold(force, column, a, b)
                column = {}
        step = step_ref[y]
        for i in range(3):
            rows = pl.ds(i * 64 + y, 8, stride=8)
            velocity = v_ref[rows, :] + force[i] * step
            new_v_ref[rows, :] = velocity
            new_u_ref[rows, :] = u_ref[rows, :] + time_step * velocity


def call(body, outs, args, unplaced=(), scratch=(), flops=1000, aliases=None):
    vmem = pl.BlockSpec(memory_space=pltpu.VMEM)
    unmoved = pl.BlockSpec(memory_space=pltpu.HBM)
    return pl.pallas_call(
        body,
        out_shape=[jax.ShapeDtypeStruct(shape, dtype) for shape, dtype in outs],
        in_specs=[unmoved if position in unplaced else vmem for position in range(len(args))],
        out_specs=[vmem for _ in outs],
        scratch_shapes=scratch,
        input_output_aliases=aliases or {},
        cost_estimate=pl.CostEstimate(flops=flops, bytes_accessed=100000, transcendentals=0),
        compiler_params=pltpu.CompilerParams(vmem_limit_bytes=16 * 1024 * 1024),
    )(
        *[
            pltpu.with_memory_space_constraint(arg, pltpu.HBM) if position in unplaced else arg
            for position, arg in enumerate(args)
        ]
    )


def along_y(down, up):
    size = lax.axis_size("gy")
    upward = [(i, i + 1) for i in range(size - 1)]
    downward = [(i + 1, i) for i in range(size - 1)]
    below = lax.ppermute(up, "gy", upward)
    above = lax.ppermute(down, "gy", downward)
    return below, above


def on_device(displacement, velocity, region, bond_words, moduli):
    copy = pltpu.SemaphoreType.DMA(())
    odd, even, u, words, region = call(
        slabs_x,
        [((SLAB, 8, LANES), F32)] * 2
        + [(x.shape, x.dtype) for x in (displacement, bond_words, region)],
        (displacement, bond_words, region),
        unplaced=(0, 1, 2),
        scratch=[copy, copy, copy],
    )
    size = lax.axis_size("gx")
    odd = lax.ppermute(odd, "gx", [(i, ((i - 1) ^ 1) + 1) for i in range(1, size - 1)])
    even = lax.ppermute(even, "gx", [(i, i ^ 1) for i in range(size)])
    even = even.reshape(SLAB * 8, LANES)
    odd = odd.reshape(SLAB * 8, LANES)
    u = u.reshape(192, LANES)
    words = words.reshape(704, LANES)
    region = region.reshape(64, LANES)
    scalars = [pltpu.SMEM(moduli.shape, F32), copy]
    displaced = ((21, UX_ROWS, LANES), F32)
    per_node = ((3, FX_ROWS, LANES), F32)
    ux, own = call(
        own_part,
        [displaced, ((24, 8, LANES), F32)],
        (u, words, region, moduli),
        unplaced=(3,),
        scratch=scalars,
        flops=10_000_000,
    )
    ux, fields, down, up = call(
        slabs_y,
        [displaced, per_node, ((SLAB_Y, LANES), F32), ((SLAB_Y, LANES), F32)],
        (u, words, own, moduli, even, odd, ux),
        unplaced=(3,),
        scratch=scalars,
        flops=10_000_000,
        aliases={6: 0},
    )
    below, above = along_y(down, up)
    fields, wx, part, balance, step = call(
        inner_force,
        [
            per_node,
            ((WORDS, WX_ROWS, LANES), jnp.int32),
            ((24, 8, LANES), F32),
            ((24, 8, LANES), F32),
            ((8, 8, LANES), F32),
        ],
        (ux, words, region, moduli, even, odd, fields),
        unplaced=(3,),
        scratch=[pltpu.VMEM((7, 16 * SU, LANES), F32)] + scalars,
        flops=40_000_000,
        aliases={6: 0},
    )
    new_u, new_v = call(
        outer_force,
        [((192, LANES), F32)] * 2,
        (
            below,
            above,
            ux,
            wx,
            fields,
            part,
            balance,
            step,
            u,
            velocity.reshape(192, LANES),
        ),
        scratch=[
            pltpu.VMEM((15, 20 * SH, LANES), F32),
            pltpu.VMEM((20 * SH, LANES), F32),
            pltpu.VMEM((5, 12 * SH, LANES), F32),
            pltpu.VMEM((7, 16 * SU, LANES), F32),
            pltpu.VMEM((24, 8, LANES), F32),
        ],
        flops=10_000_000,
    )
    return new_u.reshape(displacement.shape), new_v.reshape(velocity.shape)


def solution(mesh):
    placed = (
        P(None, "gx", "gy", None),
        P(None, "gx", "gy", None),
        P("gx", "gy", None),
        P(None, "gx", "gy", None),
        P(),
    )
    return jax.shard_map(
        on_device,
        mesh=mesh,
        in_specs=placed,
        out_specs=(P(None, "gx", "gy", None), P(None, "gx", "gy", None)),
        check_vma=False,
    )
```

```python
import math

import jax
import jax.numpy as jnp
from jax import lax
from jax.experimental import pallas as pl
from jax.experimental.pallas import tpu as pltpu
from jax.sharding import PartitionSpec as P


HORIZON = 3
time_step = 0.3
bits_per_word = 12
F32 = jnp.float32
LANES = 128

OFFSETS = [
    (a, b, c)
    for a in range(-HORIZON, HORIZON + 1)
    for b in range(-HORIZON, HORIZON + 1)
    for c in range(-HORIZON, HORIZON + 1)
    if 0 < a * a + b * b + c * c <= HORIZON * HORIZON
]
CLASSES = sorted({a * a + b * b + c * c for a, b, c in OFFSETS})
NUMBERS = {offset: number for number, offset in enumerate(OFFSETS)}
WORDS = (len(OFFSETS) + bits_per_word - 1) // bits_per_word


def square(offset):
    return offset[0] * offset[0] + offset[1] * offset[1] + offset[2] * offset[2]


UX_ROWS = 20 * 28
WX_ROWS = 16 * 18
FX_ROWS = 16 * 18
SU = 14
SH = 7
BLOCKS = (-4, 4)
EXTRA_TILE = 33
U_TILE = 36
R_TILE = 54
SLAB = 57
SLAB_Y = 246


def rolled(value, shift):
    return value if shift == 0 else pltpu.roll(value, (-shift) % LANES, 1)


def ux_rows(x, y):
    return pl.ds(((x + 6) * 14 + y + 3) * 2, 8, stride=28)


def ux_column(x, y=0):
    return pl.ds(((x + 6) * 14 + y + 3) * 2, 8, stride=2)


def fx_rows(x, y):
    return pl.ds(((x + 4) * 9 + y) * 2, 8, stride=18)


def fx_column(x):
    return pl.ds((x + 4) * 18, 8, stride=2)


def u_at(ref, component, shift, x, y):
    return ref[component * 7 + shift + 3, ux_rows(x, y), :]


def word_at(ref, k, x, y):
    return ref[k, fx_rows(x, y), :]


def uh_at(ref, component, shift, x, h):
    return ref[component * 5 + shift + 2, pl.ds((x + 6) * SH + h, 8, stride=SH), :]


def slab_u(component, depth, x):
    if depth < 2:
        return pl.ds((x + 5) * 6 + component * 2 + depth, 8, stride=6)
    return pl.ds(108 + (x + 3) * 3 + component, 8, stride=3)


def slab_field(field, depth, x):
    if depth < 2:
        return pl.ds(150 + (x + 2) * 6 + field * 2 + depth, 8, stride=6)
    return pl.ds(222 + x * 3 + field, 8, stride=3)


def slab_places(depth):
    return ((-5, 3, 5), (-2, 2)) if depth < 2 else ((-3, 3), (0,))


def scaled(value, factor):
    if factor == 1:
        return value
    if factor == -1:
        return -value
    return value * float(factor)


def combined(values, offset):
    total = None
    for value, factor in zip(values, offset):
        if factor == 0:
            continue
        if total is None:
            total = scaled(value, factor)
        elif factor == 1:
            total = total + value
        elif factor == -1:
            total = total - value
        else:
            total = total + value * float(factor)
    return total


def bit(word, number):
    return (word & (1 << (number % bits_per_word))) != 0


def add_to(store, key, value):
    store[key] = value if store.get(key) is None else store[key] + value


def by_class(store):
    total = None
    for cls, value in store.items():
        term = value * (1.0 / math.sqrt(cls))
        total = term if total is None else total + term
    return total


def chosen(region, moduli_ref, row):
    value = jnp.where(region == 1, moduli_ref[row, 1], moduli_ref[row, 0])
    value = jnp.where(region == 2, moduli_ref[row, 2], value)
    return jnp.where(region == 3, moduli_ref[row, 3], value)


def px_at(ref, shift, x, y):
    return ref[shift + 3, pl.ds((x + 4) * SU + y + 3, 8, stride=SU), :]


def field_at(ref, field, x, y):
    return ref[field, fx_rows(x, y), :]


def crossing(y):
    found = []
    for number, offset in enumerate(OFFSETS):
        target = y + offset[1]
        if target < 0:
            found.append((number, offset, target + 3))
        elif target > 7:
            found.append((number, offset, target - 8 + 3))
    return found


def slabs_x(
    u_hbm, w_hbm, r_hbm, odd_ref, even_ref, u_ref, w_ref, r_ref, u_sem, w_sem, r_sem
):
    parity = lax.axis_index("gx") % 2
    copies = [
        pltpu.make_async_copy(w_hbm, w_ref, w_sem),
        pltpu.make_async_copy(u_hbm, u_ref, u_sem),
        pltpu.make_async_copy(r_hbm, r_ref, r_sem),
    ]
    for copy in copies:
        copy.start()
    for copy in copies:
        copy.wait()
    for ref, right in ((even_ref, 1 - parity), (odd_ref, parity)):
        for k in range(WORDS):
            for d in range(3):
                ref[k * 3 + d] = w_ref[k, right * 5 + d].astype(F32)
        for d in range(3):
            ref[EXTRA_TILE + d] = w_ref[right * 8 + d, right + 3].astype(F32)
        for c in range(3):
            for d in range(6):
                ref[U_TILE + c * 6 + d] = u_ref[c, right * 2 + d]
        for d in range(3):
            ref[R_TILE + d] = r_ref[right * 5 + d].astype(F32)


def column_sum(ux_ref, words, x, inside):
    own = [ux_ref[i * 7 + 3, ux_column(x), :] for i in range(3)]
    sums = {}
    loaded = None
    for number, offset in enumerate(OFFSETS):
        if not inside(x + offset[0]):
            continue
        if loaded != number // bits_per_word:
            loaded = number // bits_per_word
            word = words(loaded)
        difference = [
            ux_ref[i * 7 + offset[2] + 3, ux_column(x + offset[0], offset[1]), :] - own[i]
            if offset[i] != 0
            else None
            for i in range(3)
        ]
        along = combined(difference, offset)
        add_to(sums, square(offset), jnp.where(bit(word, number), along, 0.0))
    return by_class(sums)


def ratios(words, region, moduli_ref):
    counts = {}
    for k in range(WORDS):
        word = words(k)
        group = OFFSETS[k * bits_per_word : (k + 1) * bits_per_word]
        for cls in CLASSES:
            held = sum(1 << i for i, offset in enumerate(group) if square(offset) == cls)
            if held:
                add_to(counts, cls, lax.population_count(word & held))
    volume = None
    for cls in CLASSES:
        term = counts[cls].astype(F32) * math.sqrt(cls)
        volume = term if volume is None else volume + term
    inverse = 1.0 / jnp.where(volume > 0.0, volume, 1.0)
    bulk = chosen(region, moduli_ref, 0)
    shear = chosen(region, moduli_ref, 1)
    return (3.0 * inverse) * ((3.0 * bulk - 5.0 * shear) * inverse), 15.0 * shear * inverse


def spread_column(ux_ref, component, x, value):
    for shift in range(-3, 4):
        ux_ref[component * 7 + shift + 3, ux_column(x), :] = rolled(value, shift)


def own_part(u_ref, w_ref, r_ref, moduli_hbm, ux_ref, own_ref, moduli_ref, moduli_sem):
    fetch = pltpu.make_async_copy(moduli_hbm, moduli_ref, moduli_sem)
    fetch.start()
    zero = jnp.zeros((8, LANES), F32)
    for i in range(3):
        for x in range(8):
            spread_column(ux_ref, i, x, u_ref[pl.ds(i * 64 + x * 8, 8), :])
        for shift in range(-2, 3):
            for y in (-3, -2, -1, 8, 9, 10):
                for x in (-6, 2, 6):
                    ux_ref[i * 7 + shift + 3, ux_rows(x, y), :] = zero
    for x in range(8):
        own_ref[x] = column_sum(
            ux_ref,
            lambda k, x=x: w_ref[pl.ds(k * 64 + x * 8, 8), :],
            x,
            lambda far: 0 <= far < 8,
        )
    fetch.wait()
    for x in range(8):
        own_ref[8 + x], own_ref[16 + x] = ratios(
            lambda k, x=x: w_ref[pl.ds(k * 64 + x * 8, 8), :],
            r_ref[pl.ds(x * 8, 8), :],
            moduli_ref,
        )


def halo_reader(even_ref, odd_ref):
    parity = lax.axis_index("gx") % 2

    def tile(index, left):
        rows = pl.ds(index * 8, 8)
        even, odd = (even_ref[rows, :], odd_ref[rows, :])
        return jnp.where(parity == 0, odd, even) if left else jnp.where(parity == 0, even, odd)

    def word(k, x):
        d = x + 3 if x < 0 else x - 8
        return tile(k * 3 + d, x < 0).astype(jnp.int32)

    def region(x):
        d = x + 3 if x < 0 else x - 8
        return tile(R_TILE + d, x < 0).astype(jnp.int32)

    return tile, word, region


def slabs_y(
    u_ref,
    w_ref,
    own_ref,
    moduli_hbm,
    even_ref,
    odd_ref,
    ux_in_ref,
    ux_ref,
    field_ref,
    down_ref,
    up_ref,
    moduli_ref,
    moduli_sem,
):
    fetch = pltpu.make_async_copy(moduli_hbm, moduli_ref, moduli_sem)
    fetch.start()
    tile, halo_word, halo_region = halo_reader(even_ref, odd_ref)
    for i in range(3):
        for d in range(6):
            spread_column(ux_ref, i, d - 6, tile(U_TILE + i * 6 + d, True))
            spread_column(ux_ref, i, d + 8, tile(U_TILE + i * 6 + d, False))
    for x in range(8):
        value = own_ref[x]
        if x < 3 or x > 4:
            value = value + column_sum(
                ux_ref,
                lambda k, x=x: w_ref[pl.ds(k * 64 + x * 8, 8), :],
                x,
                lambda far: far < 0 or far > 7,
            )
        field_ref[0, fx_column(x), :] = value
        field_ref[1, fx_column(x), :] = own_ref[8 + x]
        field_ref[2, fx_column(x), :] = own_ref[16 + x]
    for x in (-2, -1, 8, 9):
        field_ref[0, fx_column(x), :] = column_sum(
            ux_ref, lambda k, x=x: halo_word(k, x), x, lambda far: True
        )
    fetch.wait()
    for x in (-2, -1, 8, 9):
        field_ref[1, fx_column(x), :], field_ref[2, fx_column(x), :] = ratios(
            lambda k, x=x: halo_word(k, x), halo_region(x), moduli_ref
        )
    for ref, first, step in ((down_ref, 0, 1), (up_ref, 7, -1)):
        for i in range(3):
            for depth in range(3):
                y = first + step * depth
                places, field_places = slab_places(depth)
                for x in places:
                    ref[slab_u(i, depth, x), :] = u_at(ux_ref, i, 0, x, y)
                for x in field_places:
                    ref[slab_field(i, depth, x), :] = field_at(field_ref, i, x, y)


def fold(force, column, a, b):
    force = list(force)
    total = None
    for value in column.values():
        total = value if total is None else total + value
    for i, factor in ((0, a), (1, b)):
        if factor != 0:
            term = scaled(total, factor)
            force[i] = term if force[i] is None else force[i] + term
    for c, value in column.items():
        if c > 0:
            term = scaled(value - column[-c], c)
            force[2] = term if force[2] is None else force[2] + term
    return force


def halo_y(h):
    return h - 3 if h < 3 else h + 5


def inner_force(
    ux_ref,
    w_ref,
    r_ref,
    moduli_hbm,
    even_ref,
    odd_ref,
    field_in_ref,
    field_ref,
    wx_ref,
    part_ref,
    sum_ref,
    step_ref,
    hd_ref,
    weight_ref,
    sx_ref,
    moduli_ref,
    moduli_sem,
):
    fetch = pltpu.make_async_copy(moduli_hbm, moduli_ref, moduli_sem)
    fetch.start()
    tile, halo_word, halo_region = halo_reader(even_ref, odd_ref)
    for k in range(WORDS):
        for x in range(8):
            wx_ref[k, fx_column(x), :] = w_ref[pl.ds(k * 64 + x * 8, 8), :]
        for x in (-3, -2, -1, 8, 9, 10):
            wx_ref[k, fx_column(x), :] = halo_word(k, x)
    for d in range(3):
        wx_ref[8 + d, fx_column(-4), :] = tile(EXTRA_TILE + d, True).astype(jnp.int32)
        wx_ref[d, fx_column(11), :] = tile(EXTRA_TILE + d, False).astype(jnp.int32)
    zero = jnp.zeros((8, LANES), F32)
    for x in BLOCKS:
        for y in (-3, -2, -1, 8, 9, 10):
            for lead in range(1, 6):
                sx_ref[lead, pl.ds((x + 4) * SU + y + 3, 8, stride=SU), :] = zero
    for x in (-3, 10):
        field_ref[0, fx_column(x), :] = column_sum(
            ux_ref, lambda k, x=x: halo_word(k, x), x, lambda far: True
        )
    fetch.wait()
    for x in (-3, 10):
        field_ref[1, fx_column(x), :], field_ref[2, fx_column(x), :] = ratios(
            lambda k, x=x: halo_word(k, x), halo_region(x), moduli_ref
        )
    for y in range(8):
        step_ref[y] = time_step / chosen(r_ref[pl.ds(y, 8, stride=8), :], moduli_ref, 2)
        for x in BLOCKS:
            shear = field_at(field_ref, 2, x, y)
            for shift in range(-3, 4):
                sx_ref[
                    shift + 3, pl.ds((x + 4) * SU + y + 3, 8, stride=SU), :
                ] = rolled(shear, shift)

    for h in range(6):
        for x in (-6, 2, 6):
            hd_ref[pl.ds((x + 6) * SH + h, 8, stride=SH), :] = zero
    for x0 in BLOCKS:
        for h in range(6):
            for a in range(-2, 3):
                spread = None
                for c in range(-2, 3):
                    gathered = None
                    for y in range(8):
                        offset = (a, halo_y(h) - y, c)
                        if offset not in NUMBERS:
                            continue
                        number = NUMBERS[offset]
                        factor = 1.0 / math.sqrt(square(offset))
                        held = bit(word_at(wx_ref, number // bits_per_word, x0, y), number)
                        own = [
                            u_at(ux_ref, i, 0, x0, y) if offset[i] != 0 else None
                            for i in range(3)
                        ]
                        term = jnp.where(held, combined(own, offset) * factor, 0.0)
                        gathered = term if gathered is None else gathered + term
                    if gathered is not None:
                        value = rolled(gathered, -c)
                        spread = value if spread is None else spread + value
                if spread is not None:
                    rows = pl.ds((x0 + a + 6) * SH + h, 8, stride=SH)
                    hd_ref[rows, :] = hd_ref[rows, :] - spread

    def row(y, carry):
        own = [u_at(ux_ref, c, 0, 0, y) for c in range(3)]
        shear = px_at(sx_ref, 0, 0, y)
        force = [None, None, None]
        balance = [None, None, None]
        word = None
        column = {}
        count = {}
        for number, offset in enumerate(OFFSETS):
            if number % bits_per_word == 0:
                word = word_at(wx_ref, number // bits_per_word, 0, y)
            a, b, c = offset
            difference = [
                u_at(ux_ref, i, c, a, y + b) - own[i] if offset[i] != 0 else None
                for i in range(3)
            ]
            cls = square(offset)
            value = (shear + px_at(sx_ref, c, a, y + b)) * combined(difference, offset)
            held = bit(word, number)
            column[c] = jnp.where(held, value * (1.0 / (cls * math.sqrt(cls))), 0.0)
            count[c] = jnp.where(held, F32(1.0 / math.sqrt(cls)), F32(0.0))
            weight_ref[number * 8 + y] = count[c]
            if number + 1 == len(OFFSETS) or OFFSETS[number + 1][:2] != (a, b):
                force = fold(force, column, a, b)
                balance = fold(balance, count, a, b)
                column = {}
                count = {}
        for i in range(3):
            part_ref[i * 8 + y] = force[i]
            sum_ref[i * 8 + y] = balance[i]
        return carry

    lax.fori_loop(0, 8, row, 0)


def side_of(low):
    return ((0, 1, 2), -3, 4) if low else ((5, 6, 7), 5, 10)


def add_side(
    low, slab_ref, ux_ref, wx_ref, field_ref, hd_ref, weight_ref, sum_ref, uh_ref, sh_ref, px_ref
):
    edge, first, last = side_of(low)
    halo = [(depth, 2 - depth if low else 3 + depth) for depth in range(3)]
    for depth, h in halo:
        for i in range(3):
            for x in slab_places(depth)[0]:
                value = slab_ref[slab_u(i, depth, x), :]
                for shift in range(-2, 3) if depth < 2 else (0,):
                    uh_ref[
                        i * 5 + shift + 2, pl.ds((x + 6) * SH + h, 8, stride=SH), :
                    ] = rolled(value, shift)
    for depth, h in halo:
        for x in slab_places(depth)[1]:
            part, ratio, shear = [slab_ref[slab_field(i, depth, x), :] for i in range(3)]
            pressure = (part + hd_ref[pl.ds((x + 6) * SH + h, 8, stride=SH), :]) * ratio
            for shift in range(-2, 3) if depth < 2 else (0,):
                px_ref[
                    shift + 3, pl.ds((x + 4) * SU + halo_y(h) + 3, 8, stride=SU), :
                ] = rolled(pressure, shift)
                sh_ref[shift + 2, pl.ds((x + 2) * SH + h, 8, stride=SH), :] = rolled(
                    shear, shift
                )
    for y in range(max(first, 0), min(last, 7) + 1):
        for x0 in BLOCKS:
            total = field_at(field_ref, 0, x0, y)
            if y in edge:
                sums = {}
                for number, offset, h in crossing(y):
                    far = [
                        uh_at(uh_ref, i, offset[2], x0 + offset[0], h)
                        if offset[i] != 0
                        else None
                        for i in range(3)
                    ]
                    held = bit(word_at(wx_ref, number // bits_per_word, x0, y), number)
                    add_to(sums, square(offset), jnp.where(held, combined(far, offset), 0.0))
                total = total + by_class(sums)
            pressure = total * field_at(field_ref, 1, x0, y)
            for shift in range(-3, 4):
                px_ref[
                    shift + 3, pl.ds((x0 + 4) * SU + y + 3, 8, stride=SU), :
                ] = rolled(pressure, shift)

    def row(y, force):
        force = list(force)
        if y in edge:
            own = [u_at(ux_ref, c, 0, 0, y) for c in range(3)]
            shear = field_at(field_ref, 2, 0, y)
            column = {}
            bonds = crossing(y)
            for position, (number, (a, b, c), h) in enumerate(bonds):
                offset = (a, b, c)
                far = [
                    uh_at(uh_ref, i, c, a, h) if offset[i] != 0 else None for i in range(3)
                ]
                reach = combined(far, offset)
                near = combined(
                    [own[i] if offset[i] != 0 else None for i in range(3)], offset
                )
                far_shear = sh_ref[c + 2, pl.ds((a + 2) * SH + h, 8, stride=SH), :]
                value = far_shear * (reach - near) + shear * reach
                column[c] = (value * (1.0 / square(offset))) * weight_ref[number * 8 + y]
                if position + 1 == len(bonds) or bonds[position + 1][1][:2] != (a, b):
                    force = fold(force, column, a, b)
                    column = {}
        if first <= y <= last:
            pressure = px_at(px_ref, 0, 0, y)
            force = [force[i] + pressure * sum_ref[i * 8 + y] for i in range(3)]
        column = {}
        for number, (a, b, c) in enumerate(OFFSETS):
            if not first <= y + b <= last:
                continue
            column[c] = px_at(px_ref, c, a, y + b) * weight_ref[number * 8 + y]
            if number + 1 == len(OFFSETS) or OFFSETS[number + 1][:2] != (a, b):
                force = fold(force, column, a, b)
                column = {}
        return force

    return row


def lower_force(
    slab_ref,
    ux_ref,
    wx_ref,
    field_ref,
    hd_ref,
    weight_ref,
    sum_ref,
    part_ref,
    force_ref,
    uh_ref,
    sh_ref,
    px_ref,
):
    row = add_side(
        True, slab_ref, ux_ref, wx_ref, field_ref, hd_ref, weight_ref, sum_ref, uh_ref, sh_ref, px_ref
    )
    for y in range(8):
        force = row(y, [part_ref[i * 8 + y] for i in range(3)])
        for i in range(3):
            force_ref[i * 8 + y] = force[i]


def outer_force(
    slab_ref,
    ux_ref,
    wx_ref,
    field_ref,
    hd_ref,
    weight_ref,
    sum_ref,
    force_ref,
    step_ref,
    u_ref,
    v_ref,
    new_u_ref,
    new_v_ref,
    uh_ref,
    sh_ref,
    px_ref,
):
    row = add_side(
        False, slab_ref, ux_ref, wx_ref, field_ref, hd_ref, weight_ref, sum_ref, uh_ref, sh_ref, px_ref
    )
    for y in range(8):
        force = row(y, [force_ref[i * 8 + y] for i in range(3)])
        for i in range(3):
            rows = pl.ds(i * 64 + y, 8, stride=8)
            velocity = v_ref[rows, :] + force[i] * step_ref[y]
            new_v_ref[rows, :] = velocity
            new_u_ref[rows, :] = u_ref[rows, :] + time_step * velocity


def call(body, outs, args, unplaced=(), scratch=(), flops=1000, aliases=None):
    vmem = pl.BlockSpec(memory_space=pltpu.VMEM)
    unmoved = pl.BlockSpec(memory_space=pltpu.HBM)
    return pl.pallas_call(
        body,
        out_shape=[jax.ShapeDtypeStruct(shape, dtype) for shape, dtype in outs],
        in_specs=[unmoved if position in unplaced else vmem for position in range(len(args))],
        out_specs=[vmem for _ in outs],
        scratch_shapes=scratch,
        input_output_aliases=aliases or {},
        cost_estimate=pl.CostEstimate(flops=flops, bytes_accessed=100000, transcendentals=0),
        compiler_params=pltpu.CompilerParams(vmem_limit_bytes=16 * 1024 * 1024),
    )(
        *[
            pltpu.with_memory_space_constraint(arg, pltpu.HBM) if position in unplaced else arg
            for position, arg in enumerate(args)
        ]
    )


def along_y(down, up):
    size = lax.axis_size("gy")
    upward = [(i, i + 1) for i in range(size - 1)]
    downward = [(i + 1, i) for i in range(size - 1)]
    below = lax.ppermute(up, "gy", upward)
    above = lax.ppermute(down, "gy", downward)
    return below, above


def on_device(displacement, velocity, region, bond_words, moduli):
    copy = pltpu.SemaphoreType.DMA(())
    odd, even, u, words, region = call(
        slabs_x,
        [((SLAB, 8, LANES), F32)] * 2
        + [(x.shape, x.dtype) for x in (displacement, bond_words, region)],
        (displacement, bond_words, region),
        unplaced=(0, 1, 2),
        scratch=[copy, copy, copy],
    )
    size = lax.axis_size("gx")
    odd = lax.ppermute(
        odd, "gx", [(i, ((i - 1) ^ 1) + 1) for i in range(1, size - 1)]
    )
    even = lax.ppermute(even, "gx", [(i, i ^ 1) for i in range(size)])
    even = even.reshape(SLAB * 8, LANES)
    odd = odd.reshape(SLAB * 8, LANES)
    u = u.reshape(192, LANES)
    words = words.reshape(704, LANES)
    region = region.reshape(64, LANES)
    scalars = [pltpu.SMEM(moduli.shape, F32), copy]
    displaced = ((21, UX_ROWS, LANES), F32)
    per_node = ((3, FX_ROWS, LANES), F32)
    ux, own = call(
        own_part,
        [displaced, ((24, 8, LANES), F32)],
        (u, words, region, moduli),
        unplaced=(3,),
        scratch=scalars,
        flops=10_000_000,
    )
    ux, fields, down, up = call(
        slabs_y,
        [displaced, per_node, ((SLAB_Y, LANES), F32), ((SLAB_Y, LANES), F32)],
        (u, words, own, moduli, even, odd, ux),
        unplaced=(3,),
        scratch=scalars,
        flops=10_000_000,
        aliases={6: 0},
    )
    below, above = along_y(down, up)
    fields, wx, part, balance, step, halo, weights = call(
        inner_force,
        [
            per_node,
            ((WORDS, WX_ROWS, LANES), jnp.int32),
            ((24, 8, LANES), F32),
            ((24, 8, LANES), F32),
            ((8, 8, LANES), F32),
            ((20 * SH, LANES), F32),
            ((len(OFFSETS) * 8, 8, LANES), F32),
        ],
        (ux, words, region, moduli, even, odd, fields),
        unplaced=(3,),
        scratch=[pltpu.VMEM((7, 16 * SU, LANES), F32)] + scalars,
        flops=40_000_000,
        aliases={6: 0},
    )
    shared = (ux, wx, fields, halo, weights, balance)
    working = [
        pltpu.VMEM((15, 20 * SH, LANES), F32),
        pltpu.VMEM((5, 12 * SH, LANES), F32),
        pltpu.VMEM((7, 16 * SU, LANES), F32),
    ]
    (force,) = call(
        lower_force,
        [((24, 8, LANES), F32)],
        (below,) + shared + (part,),
        scratch=working,
        flops=10_000_000,
    )
    new_u, new_v = call(
        outer_force,
        [((192, LANES), F32)] * 2,
        (above,) + shared + (force, step, u, velocity.reshape(192, LANES)),
        scratch=working,
        flops=10_000_000,
    )
    return new_u.reshape(displacement.shape), new_v.reshape(velocity.shape)


def solution(mesh):
    placed = (
        P(None, "gx", "gy", None),
        P(None, "gx", "gy", None),
        P("gx", "gy", None),
        P(None, "gx", "gy", None),
        P(),
    )
    return jax.shard_map(
        on_device,
        mesh=mesh,
        in_specs=placed,
        out_specs=(P(None, "gx", "gy", None), P(None, "gx", "gy", None)),
        check_vma=False,
    )
```

```python
import math

import jax
import jax.numpy as jnp
from jax import lax
from jax.experimental import pallas as pl
from jax.experimental.pallas import tpu as pltpu
from jax.sharding import PartitionSpec as P


HORIZON = 3
time_step = 0.3
bits_per_word = 12
F32 = jnp.float32
LANES = 128

OFFSETS = [
    (a, b, c)
    for a in range(-HORIZON, HORIZON + 1)
    for b in range(-HORIZON, HORIZON + 1)
    for c in range(-HORIZON, HORIZON + 1)
    if 0 < a * a + b * b + c * c <= HORIZON * HORIZON
]
CLASSES = sorted({a * a + b * b + c * c for a, b, c in OFFSETS})
NUMBERS = {offset: number for number, offset in enumerate(OFFSETS)}
WORDS = (len(OFFSETS) + bits_per_word - 1) // bits_per_word


def square(offset):
    return offset[0] * offset[0] + offset[1] * offset[1] + offset[2] * offset[2]


UX_ROWS = 20 * 28
WX_ROWS = 16 * 18
FX_ROWS = 16 * 18
SU = 14
SH = 7
BLOCKS = (-4, 4)
EXTRA_TILE = 33
U_TILE = 36
R_TILE = 52
SLAB = 55
SLAB_Y = 218


def rolled(value, shift):
    return value if shift == 0 else pltpu.roll(value, (-shift) % LANES, 1)


def ux_rows(x, y):
    return pl.ds(((x + 6) * 14 + y + 3) * 2, 8, stride=28)


def ux_column(x, y=0):
    return pl.ds(((x + 6) * 14 + y + 3) * 2, 8, stride=2)


def fx_rows(x, y):
    return pl.ds(((x + 4) * 9 + y) * 2, 8, stride=18)


def fx_column(x):
    return pl.ds((x + 4) * 18, 8, stride=2)


def u_at(ref, component, shift, x, y):
    return ref[component * 7 + shift + 3, ux_rows(x, y), :]


def word_at(ref, k, x, y):
    return ref[k, fx_rows(x, y), :]


def uh_at(ref, component, shift, x, h):
    return ref[component * 5 + shift + 2, pl.ds((x + 6) * SH + h, 8, stride=SH), :]


def slab_u(component, depth, x):
    if depth < 2:
        return pl.ds((x + 5) * 6 + component * 2 + depth, 8, stride=6)
    return pl.ds(108 + x + 3, 8)


def slab_field(field, depth, x):
    if depth < 2:
        return pl.ds(122 + (x + 2) * 6 + field * 2 + depth, 8, stride=6)
    return pl.ds(194 + x * 3 + field, 8, stride=3)


def slab_components(depth):
    return range(3) if depth < 2 else (1,)


def slab_places(depth):
    return ((-5, 3, 5), (-2, 2)) if depth < 2 else ((-3, 3), (0,))


def scaled(value, factor):
    if factor == 1:
        return value
    if factor == -1:
        return -value
    return value * float(factor)


def combined(values, offset):
    total = None
    for value, factor in zip(values, offset):
        if factor == 0:
            continue
        if total is None:
            total = scaled(value, factor)
        elif factor == 1:
            total = total + value
        elif factor == -1:
            total = total - value
        else:
            total = total + value * float(factor)
    return total


def bit(word, number):
    return (word & (1 << (number % bits_per_word))) != 0


def add_to(store, key, value):
    store[key] = value if store.get(key) is None else store[key] + value


def by_class(store):
    total = None
    for cls, value in store.items():
        term = value * (1.0 / math.sqrt(cls))
        total = term if total is None else total + term
    return total


def chosen(region, moduli_ref, row):
    value = jnp.where(region == 1, moduli_ref[row, 1], moduli_ref[row, 0])
    value = jnp.where(region == 2, moduli_ref[row, 2], value)
    return jnp.where(region == 3, moduli_ref[row, 3], value)


def px_at(ref, shift, x, y):
    return ref[shift + 3, pl.ds((x + 4) * SU + y + 3, 8, stride=SU), :]


def field_at(ref, field, x, y):
    return ref[field, fx_rows(x, y), :]


def crossing(y):
    found = []
    for number, offset in enumerate(OFFSETS):
        target = y + offset[1]
        if target < 0:
            found.append((number, offset, target + 3))
        elif target > 7:
            found.append((number, offset, target - 8 + 3))
    return found


def u_depth(component):
    return 6 if component == 0 else 5


def u_tile(component):
    return U_TILE + (0 if component == 0 else 1 + component * 5)


def slabs_x(
    u_hbm, w_hbm, r_hbm, odd_ref, even_ref, u_ref, w_ref, r_ref, u_sem, w_sem, r_sem
):
    parity = lax.axis_index("gx") % 2
    copies = [
        pltpu.make_async_copy(w_hbm, w_ref, w_sem),
        pltpu.make_async_copy(u_hbm, u_ref, u_sem),
        pltpu.make_async_copy(r_hbm, r_ref, r_sem),
    ]
    for copy in copies:
        copy.start()
    for copy in copies:
        copy.wait()
    for ref, right in ((even_ref, 1 - parity), (odd_ref, parity)):
        for k in range(WORDS):
            for d in range(3):
                ref[k * 3 + d] = w_ref[k, right * 5 + d].astype(F32)
        for d in range(3):
            ref[EXTRA_TILE + d] = w_ref[right * 8 + d, right + 3].astype(F32)
        for c in range(3):
            for d in range(u_depth(c)):
                ref[u_tile(c) + d] = u_ref[c, right * (8 - u_depth(c)) + d]
        for d in range(3):
            ref[R_TILE + d] = r_ref[right * 5 + d].astype(F32)


def column_sum(ux_ref, words, x, inside):
    own = [ux_ref[i * 7 + 3, ux_column(x), :] for i in range(3)]
    sums = {}
    loaded = None
    for number, offset in enumerate(OFFSETS):
        if not inside(x + offset[0]):
            continue
        if loaded != number // bits_per_word:
            loaded = number // bits_per_word
            word = words(loaded)
        difference = [
            ux_ref[i * 7 + offset[2] + 3, ux_column(x + offset[0], offset[1]), :] - own[i]
            if offset[i] != 0
            else None
            for i in range(3)
        ]
        along = combined(difference, offset)
        add_to(sums, square(offset), jnp.where(bit(word, number), along, 0.0))
    return by_class(sums)


def ratios(words, region, moduli_ref):
    counts = {}
    for k in range((WORDS + 1) // 2):
        word = words(k) if k < WORDS // 2 else words(WORDS - 1)
        group = OFFSETS[k * bits_per_word : (k + 1) * bits_per_word]
        if k < WORDS // 2:
            other = WORDS - 2 - k
            word = word | (words(other) << bits_per_word)
            group = group + OFFSETS[other * bits_per_word : (other + 1) * bits_per_word]
        else:
            group = OFFSETS[(WORDS - 1) * bits_per_word :]
        for cls in CLASSES:
            held = sum(1 << i for i, offset in enumerate(group) if square(offset) == cls)
            if held:
                add_to(counts, cls, lax.population_count(word & held))
    volume = None
    for cls in CLASSES:
        term = counts[cls].astype(F32) * math.sqrt(cls)
        volume = term if volume is None else volume + term
    inverse = 1.0 / jnp.where(volume > 0.0, volume, 1.0)
    bulk = chosen(region, moduli_ref, 0)
    shear = chosen(region, moduli_ref, 1)
    return (3.0 * inverse) * ((3.0 * bulk - 5.0 * shear) * inverse), 15.0 * shear * inverse


def spread_column(ux_ref, component, x, value):
    depth = max(-x, x - 7, 0)
    reach = 3 if depth < 4 else 2 if depth < 6 else 0
    for shift in range(-reach, reach + 1):
        ux_ref[component * 7 + shift + 3, ux_column(x), :] = rolled(value, shift)


def own_part(u_ref, w_ref, r_ref, moduli_hbm, ux_ref, own_ref, moduli_ref, moduli_sem):
    fetch = pltpu.make_async_copy(moduli_hbm, moduli_ref, moduli_sem)
    fetch.start()
    zero = jnp.zeros((8, LANES), F32)
    for i in range(3):
        for x in range(8):
            spread_column(ux_ref, i, x, u_ref[pl.ds(i * 64 + x * 8, 8), :])
        for shift in range(-2, 3):
            for y in (-3, -2, -1, 8, 9, 10):
                for x in (-6, 2, 6):
                    ux_ref[i * 7 + shift + 3, ux_rows(x, y), :] = zero
    for x in range(8):
        own_ref[x] = column_sum(
            ux_ref,
            lambda k, x=x: w_ref[pl.ds(k * 64 + x * 8, 8), :],
            x,
            lambda far: 0 <= far < 8,
        )
    fetch.wait()
    for x in range(8):
        own_ref[8 + x], own_ref[16 + x] = ratios(
            lambda k, x=x: w_ref[pl.ds(k * 64 + x * 8, 8), :],
            r_ref[pl.ds(x * 8, 8), :],
            moduli_ref,
        )


def halo_reader(even_ref, odd_ref):
    parity = lax.axis_index("gx") % 2

    def tile(index, left):
        rows = pl.ds(index * 8, 8)
        even, odd = (even_ref[rows, :], odd_ref[rows, :])
        return jnp.where(parity == 0, odd, even) if left else jnp.where(parity == 0, even, odd)

    def word(k, x):
        d = x + 3 if x < 0 else x - 8
        return tile(k * 3 + d, x < 0).astype(jnp.int32)

    def region(x):
        d = x + 3 if x < 0 else x - 8
        return tile(R_TILE + d, x < 0).astype(jnp.int32)

    return tile, word, region


def slabs_y(
    u_ref,
    w_ref,
    own_ref,
    moduli_hbm,
    even_ref,
    odd_ref,
    ux_in_ref,
    ux_ref,
    field_ref,
    down_ref,
    up_ref,
    moduli_ref,
    moduli_sem,
):
    fetch = pltpu.make_async_copy(moduli_hbm, moduli_ref, moduli_sem)
    fetch.start()
    tile, halo_word, halo_region = halo_reader(even_ref, odd_ref)
    for i in range(3):
        size = u_depth(i)
        for d in range(size):
            spread_column(ux_ref, i, d - size, tile(u_tile(i) + d, True))
            spread_column(ux_ref, i, d + 8, tile(u_tile(i) + d, False))
    for x in range(8):
        value = own_ref[x]
        if x < 3 or x > 4:
            value = value + column_sum(
                ux_ref,
                lambda k, x=x: w_ref[pl.ds(k * 64 + x * 8, 8), :],
                x,
                lambda far: far < 0 or far > 7,
            )
        field_ref[0, fx_column(x), :] = value
        field_ref[1, fx_column(x), :] = own_ref[8 + x]
        field_ref[2, fx_column(x), :] = own_ref[16 + x]
    for x in (-2, -1, 8, 9):
        field_ref[0, fx_column(x), :] = column_sum(
            ux_ref, lambda k, x=x: halo_word(k, x), x, lambda far: True
        )
    fetch.wait()
    for x in (-2, -1, 8, 9):
        field_ref[1, fx_column(x), :], field_ref[2, fx_column(x), :] = ratios(
            lambda k, x=x: halo_word(k, x), halo_region(x), moduli_ref
        )
    for ref, first, step in ((down_ref, 0, 1), (up_ref, 7, -1)):
        for depth in range(3):
            y = first + step * depth
            places, field_places = slab_places(depth)
            for i in slab_components(depth):
                for x in places:
                    ref[slab_u(i, depth, x), :] = u_at(ux_ref, i, 0, x, y)
            for i in range(3):
                for x in field_places:
                    ref[slab_field(i, depth, x), :] = field_at(field_ref, i, x, y)


def fold(force, column, a, b):
    force = list(force)
    total = None
    for value in column.values():
        total = value if total is None else total + value
    for i, factor in ((0, a), (1, b)):
        if factor != 0:
            term = scaled(total, factor)
            force[i] = term if force[i] is None else force[i] + term
    for c, value in column.items():
        if c > 0:
            term = scaled(value - column[-c], c)
            force[2] = term if force[2] is None else force[2] + term
    return force


def halo_y(h):
    return h - 3 if h < 3 else h + 5


def inner_force(
    ux_ref,
    w_ref,
    r_ref,
    moduli_hbm,
    even_ref,
    odd_ref,
    field_in_ref,
    field_ref,
    wx_ref,
    part_ref,
    sum_ref,
    step_ref,
    hd_ref,
    weight_ref,
    sx_ref,
    moduli_ref,
    moduli_sem,
):
    fetch = pltpu.make_async_copy(moduli_hbm, moduli_ref, moduli_sem)
    fetch.start()
    tile, halo_word, halo_region = halo_reader(even_ref, odd_ref)
    for k in range(WORDS):
        for x in range(8):
            wx_ref[k, fx_column(x), :] = w_ref[pl.ds(k * 64 + x * 8, 8), :]
        for x in (-3, -2, -1, 8, 9, 10):
            wx_ref[k, fx_column(x), :] = halo_word(k, x)
    for d in range(3):
        wx_ref[8 + d, fx_column(-4), :] = tile(EXTRA_TILE + d, True).astype(jnp.int32)
        wx_ref[d, fx_column(11), :] = tile(EXTRA_TILE + d, False).astype(jnp.int32)
    zero = jnp.zeros((8, LANES), F32)
    for x in BLOCKS:
        for y in (-3, -2, -1, 8, 9, 10):
            for lead in range(1, 6):
                sx_ref[lead, pl.ds((x + 4) * SU + y + 3, 8, stride=SU), :] = zero
    for x in (-3, 10):
        field_ref[0, fx_column(x), :] = column_sum(
            ux_ref, lambda k, x=x: halo_word(k, x), x, lambda far: True
        )
    fetch.wait()
    for x in (-3, 10):
        field_ref[1, fx_column(x), :], field_ref[2, fx_column(x), :] = ratios(
            lambda k, x=x: halo_word(k, x), halo_region(x), moduli_ref
        )
    for y in range(8):
        step_ref[y] = time_step / chosen(r_ref[pl.ds(y, 8, stride=8), :], moduli_ref, 2)
        for x in BLOCKS:
            shear = field_at(field_ref, 2, x, y)
            for shift in range(-3, 4):
                sx_ref[
                    shift + 3, pl.ds((x + 4) * SU + y + 3, 8, stride=SU), :
                ] = rolled(shear, shift)

    for h in range(6):
        for x in (-6, 2, 6):
            hd_ref[pl.ds((x + 6) * SH + h, 8, stride=SH), :] = zero
    for x0 in BLOCKS:
        for h in range(6):
            for a in range(-2, 3):
                spread = None
                for c in range(-2, 3):
                    gathered = None
                    for y in range(8):
                        offset = (a, halo_y(h) - y, c)
                        if offset not in NUMBERS:
                            continue
                        number = NUMBERS[offset]
                        factor = 1.0 / math.sqrt(square(offset))
                        held = bit(word_at(wx_ref, number // bits_per_word, x0, y), number)
                        own = [
                            u_at(ux_ref, i, 0, x0, y) if offset[i] != 0 else None
                            for i in range(3)
                        ]
                        term = jnp.where(held, combined(own, offset) * factor, 0.0)
                        gathered = term if gathered is None else gathered + term
                    if gathered is not None:
                        value = rolled(gathered, -c)
                        spread = value if spread is None else spread + value
                if spread is not None:
                    rows = pl.ds((x0 + a + 6) * SH + h, 8, stride=SH)
                    hd_ref[rows, :] = hd_ref[rows, :] - spread

    def row(y, carry):
        own = [u_at(ux_ref, c, 0, 0, y) for c in range(3)]
        shear = px_at(sx_ref, 0, 0, y)
        force = [None, None, None]
        balance = [None, None, None]
        word = None
        column = {}
        count = {}
        for number, offset in enumerate(OFFSETS):
            if number % bits_per_word == 0:
                word = word_at(wx_ref, number // bits_per_word, 0, y)
            a, b, c = offset
            difference = [
                u_at(ux_ref, i, c, a, y + b) - own[i] if offset[i] != 0 else None
                for i in range(3)
            ]
            cls = square(offset)
            value = (shear + px_at(sx_ref, c, a, y + b)) * combined(difference, offset)
            held = bit(word, number)
            column[c] = jnp.where(held, value * (1.0 / (cls * math.sqrt(cls))), 0.0)
            count[c] = jnp.where(held, F32(1.0 / math.sqrt(cls)), F32(0.0))
            weight_ref[number * 8 + y] = count[c]
            if number + 1 == len(OFFSETS) or OFFSETS[number + 1][:2] != (a, b):
                force = fold(force, column, a, b)
                balance = fold(balance, count, a, b)
                column = {}
                count = {}
        for i in range(3):
            part_ref[i * 8 + y] = force[i]
            sum_ref[i * 8 + y] = balance[i]
        return carry

    lax.fori_loop(0, 8, row, 0)


def side_of(low):
    return ((0, 1, 2), -3, 4) if low else ((5, 6, 7), 5, 10)


def add_side(
    low, slab_ref, ux_ref, wx_ref, field_ref, hd_ref, weight_ref, sum_ref, uh_ref, sh_ref, px_ref
):
    edge, first, last = side_of(low)
    halo = [(depth, 2 - depth if low else 3 + depth) for depth in range(3)]
    for depth, h in halo:
        for i in slab_components(depth):
            for x in slab_places(depth)[0]:
                value = slab_ref[slab_u(i, depth, x), :]
                for shift in range(-2, 3) if depth < 2 else (0,):
                    uh_ref[
                        i * 5 + shift + 2, pl.ds((x + 6) * SH + h, 8, stride=SH), :
                    ] = rolled(value, shift)
    for depth, h in halo:
        for x in slab_places(depth)[1]:
            part, ratio, shear = [slab_ref[slab_field(i, depth, x), :] for i in range(3)]
            pressure = (part + hd_ref[pl.ds((x + 6) * SH + h, 8, stride=SH), :]) * ratio
            for shift in range(-2, 3) if depth < 2 else (0,):
                px_ref[
                    shift + 3, pl.ds((x + 4) * SU + halo_y(h) + 3, 8, stride=SU), :
                ] = rolled(pressure, shift)
                sh_ref[shift + 2, pl.ds((x + 2) * SH + h, 8, stride=SH), :] = rolled(
                    shear, shift
                )
    for y in range(max(first, 0), min(last, 7) + 1):
        for x0 in BLOCKS:
            total = field_at(field_ref, 0, x0, y)
            if y in edge:
                sums = {}
                for number, offset, h in crossing(y):
                    far = [
                        uh_at(uh_ref, i, offset[2], x0 + offset[0], h)
                        if offset[i] != 0
                        else None
                        for i in range(3)
                    ]
                    held = bit(word_at(wx_ref, number // bits_per_word, x0, y), number)
                    add_to(sums, square(offset), jnp.where(held, combined(far, offset), 0.0))
                total = total + by_class(sums)
            pressure = total * field_at(field_ref, 1, x0, y)
            for shift in range(-3, 4):
                px_ref[
                    shift + 3, pl.ds((x0 + 4) * SU + y + 3, 8, stride=SU), :
                ] = rolled(pressure, shift)

    def row(y, force):
        force = list(force)
        if y in edge:
            own = [u_at(ux_ref, c, 0, 0, y) for c in range(3)]
            shear = field_at(field_ref, 2, 0, y)
            column = {}
            bonds = crossing(y)
            for position, (number, (a, b, c), h) in enumerate(bonds):
                offset = (a, b, c)
                far = [
                    uh_at(uh_ref, i, c, a, h) if offset[i] != 0 else None for i in range(3)
                ]
                reach = combined(far, offset)
                near = combined(
                    [own[i] if offset[i] != 0 else None for i in range(3)], offset
                )
                far_shear = sh_ref[c + 2, pl.ds((a + 2) * SH + h, 8, stride=SH), :]
                value = far_shear * (reach - near) + shear * reach
                column[c] = (value * (1.0 / square(offset))) * weight_ref[number * 8 + y]
                if position + 1 == len(bonds) or bonds[position + 1][1][:2] != (a, b):
                    force = fold(force, column, a, b)
                    column = {}
        if first <= y <= last:
            pressure = px_at(px_ref, 0, 0, y)
            force = [force[i] + pressure * sum_ref[i * 8 + y] for i in range(3)]
        column = {}
        for number, (a, b, c) in enumerate(OFFSETS):
            if not first <= y + b <= last:
                continue
            column[c] = px_at(px_ref, c, a, y + b) * weight_ref[number * 8 + y]
            if number + 1 == len(OFFSETS) or OFFSETS[number + 1][:2] != (a, b):
                force = fold(force, column, a, b)
                column = {}
        return force

    return row


def lower_force(
    slab_ref,
    ux_ref,
    wx_ref,
    field_ref,
    hd_ref,
    weight_ref,
    sum_ref,
    part_ref,
    force_ref,
    uh_ref,
    sh_ref,
    px_ref,
):
    row = add_side(
        True, slab_ref, ux_ref, wx_ref, field_ref, hd_ref, weight_ref, sum_ref, uh_ref, sh_ref, px_ref
    )
    for y in range(8):
        force = row(y, [part_ref[i * 8 + y] for i in range(3)])
        for i in range(3):
            force_ref[i * 8 + y] = force[i]


def outer_force(
    slab_ref,
    ux_ref,
    wx_ref,
    field_ref,
    hd_ref,
    weight_ref,
    sum_ref,
    force_ref,
    step_ref,
    u_ref,
    v_ref,
    new_u_ref,
    new_v_ref,
    uh_ref,
    sh_ref,
    px_ref,
):
    row = add_side(
        False, slab_ref, ux_ref, wx_ref, field_ref, hd_ref, weight_ref, sum_ref, uh_ref, sh_ref, px_ref
    )
    for y in range(8):
        force = row(y, [force_ref[i * 8 + y] for i in range(3)])
        for i in range(3):
            rows = pl.ds(i * 64 + y, 8, stride=8)
            velocity = v_ref[rows, :] + force[i] * step_ref[y]
            new_v_ref[rows, :] = velocity
            new_u_ref[rows, :] = u_ref[rows, :] + time_step * velocity


def call(body, outs, args, unplaced=(), scratch=(), flops=1000, aliases=None):
    vmem = pl.BlockSpec(memory_space=pltpu.VMEM)
    unmoved = pl.BlockSpec(memory_space=pltpu.HBM)
    return pl.pallas_call(
        body,
        out_shape=[jax.ShapeDtypeStruct(shape, dtype) for shape, dtype in outs],
        in_specs=[unmoved if position in unplaced else vmem for position in range(len(args))],
        out_specs=[vmem for _ in outs],
        scratch_shapes=scratch,
        input_output_aliases=aliases or {},
        cost_estimate=pl.CostEstimate(flops=flops, bytes_accessed=100000, transcendentals=0),
        compiler_params=pltpu.CompilerParams(vmem_limit_bytes=16 * 1024 * 1024),
    )(
        *[
            pltpu.with_memory_space_constraint(arg, pltpu.HBM) if position in unplaced else arg
            for position, arg in enumerate(args)
        ]
    )


def along_y(down, up):
    size = lax.axis_size("gy")
    upward = [(i, i + 1) for i in range(size - 1)]
    downward = [(i + 1, i) for i in range(size - 1)]
    below = lax.ppermute(up, "gy", upward)
    above = lax.ppermute(down, "gy", downward)
    return below, above


def on_device(displacement, velocity, region, bond_words, moduli):
    copy = pltpu.SemaphoreType.DMA(())
    odd, even, u, words, region = call(
        slabs_x,
        [((SLAB, 8, LANES), F32)] * 2
        + [(x.shape, x.dtype) for x in (displacement, bond_words, region)],
        (displacement, bond_words, region),
        unplaced=(0, 1, 2),
        scratch=[copy, copy, copy],
    )
    size = lax.axis_size("gx")
    odd = lax.ppermute(
        odd, "gx", [(i, ((i - 1) ^ 1) + 1) for i in range(1, size - 1)]
    )
    even = lax.ppermute(even, "gx", [(i, i ^ 1) for i in range(size)])
    even = even.reshape(SLAB * 8, LANES)
    odd = odd.reshape(SLAB * 8, LANES)
    u = u.reshape(192, LANES)
    words = words.reshape(704, LANES)
    region = region.reshape(64, LANES)
    scalars = [pltpu.SMEM(moduli.shape, F32), copy]
    displaced = ((21, UX_ROWS, LANES), F32)
    per_node = ((3, FX_ROWS, LANES), F32)
    ux, own = call(
        own_part,
        [displaced, ((24, 8, LANES), F32)],
        (u, words, region, moduli),
        unplaced=(3,),
        scratch=scalars,
        flops=10_000_000,
    )
    ux, fields, down, up = call(
        slabs_y,
        [displaced, per_node, ((SLAB_Y, LANES), F32), ((SLAB_Y, LANES), F32)],
        (u, words, own, moduli, even, odd, ux),
        unplaced=(3,),
        scratch=scalars,
        flops=10_000_000,
        aliases={6: 0},
    )
    below, above = along_y(down, up)
    fields, wx, part, balance, step, halo, weights = call(
        inner_force,
        [
            per_node,
            ((WORDS, WX_ROWS, LANES), jnp.int32),
            ((24, 8, LANES), F32),
            ((24, 8, LANES), F32),
            ((8, 8, LANES), F32),
            ((20 * SH, LANES), F32),
            ((len(OFFSETS) * 8, 8, LANES), F32),
        ],
        (ux, words, region, moduli, even, odd, fields),
        unplaced=(3,),
        scratch=[pltpu.VMEM((7, 16 * SU, LANES), F32)] + scalars,
        flops=40_000_000,
        aliases={6: 0},
    )
    shared = (ux, wx, fields, halo, weights, balance)
    working = [
        pltpu.VMEM((15, 20 * SH, LANES), F32),
        pltpu.VMEM((5, 12 * SH, LANES), F32),
        pltpu.VMEM((7, 16 * SU, LANES), F32),
    ]
    (force,) = call(
        lower_force,
        [((24, 8, LANES), F32)],
        (below,) + shared + (part,),
        scratch=working,
        flops=10_000_000,
    )
    new_u, new_v = call(
        outer_force,
        [((192, LANES), F32)] * 2,
        (above,) + shared + (force, step, u, velocity.reshape(192, LANES)),
        scratch=working,
        flops=10_000_000,
    )
    return new_u.reshape(displacement.shape), new_v.reshape(velocity.shape)


def solution(mesh):
    placed = (
        P(None, "gx", "gy", None),
        P(None, "gx", "gy", None),
        P("gx", "gy", None),
        P(None, "gx", "gy", None),
        P(),
    )
    return jax.shard_map(
        on_device,
        mesh=mesh,
        in_specs=placed,
        out_specs=(P(None, "gx", "gy", None), P(None, "gx", "gy", None)),
        check_vma=False,
    )
```

```python
import math

import jax
import jax.numpy as jnp
from jax import lax
from jax.experimental import pallas as pl
from jax.experimental.pallas import tpu as pltpu
from jax.sharding import PartitionSpec as P


HORIZON = 3
time_step = 0.3
bits_per_word = 12
F32 = jnp.float32
LANES = 128

OFFSETS = [
    (a, b, c)
    for a in range(-HORIZON, HORIZON + 1)
    for b in range(-HORIZON, HORIZON + 1)
    for c in range(-HORIZON, HORIZON + 1)
    if 0 < a * a + b * b + c * c <= HORIZON * HORIZON
]
CLASSES = sorted({a * a + b * b + c * c for a, b, c in OFFSETS})
NUMBERS = {offset: number for number, offset in enumerate(OFFSETS)}
WORDS = (len(OFFSETS) + bits_per_word - 1) // bits_per_word


def square(offset):
    return offset[0] * offset[0] + offset[1] * offset[1] + offset[2] * offset[2]


UX_ROWS = 20 * 28
WX_ROWS = 16 * 18
FX_ROWS = 16 * 18
SU = 14
SH = 7
BLOCKS = (-4, 4)
EXTRA_TILE = 33
U_TILE = 36
R_TILE = 52
SLAB = 55
SLAB_Y = 218


def rolled(value, shift):
    return value if shift == 0 else pltpu.roll(value, (-shift) % LANES, 1)


def ux_rows(x, y):
    return pl.ds(((x + 6) * 14 + y + 3) * 2, 8, stride=28)


def ux_column(x, y=0):
    return pl.ds(((x + 6) * 14 + y + 3) * 2, 8, stride=2)


def fx_rows(x, y):
    return pl.ds(((x + 4) * 9 + y) * 2, 8, stride=18)


def fx_column(x):
    return pl.ds((x + 4) * 18, 8, stride=2)


def u_at(ref, component, shift, x, y):
    return ref[component * 7 + shift + 3, ux_rows(x, y), :]


def word_at(ref, k, x, y):
    return ref[k, fx_rows(x, y), :]


def uh_at(ref, component, shift, x, h):
    return ref[component * 5 + shift + 2, pl.ds((x + 6) * SH + h, 8, stride=SH), :]


def slab_u(component, depth, x):
    if depth < 2:
        return pl.ds((x + 5) * 6 + component * 2 + depth, 8, stride=6)
    return pl.ds(108 + x + 3, 8)


def slab_field(field, depth, x):
    if depth < 2:
        return pl.ds(122 + (x + 2) * 6 + field * 2 + depth, 8, stride=6)
    return pl.ds(194 + x * 3 + field, 8, stride=3)


def slab_components(depth):
    return range(3) if depth < 2 else (1,)


def slab_places(depth):
    return ((-5, 3, 5), (-2, 2)) if depth < 2 else ((-3, 3), (0,))


def scaled(value, factor):
    if factor == 1:
        return value
    if factor == -1:
        return -value
    return value * float(factor)


def combined(values, offset):
    total = None
    for value, factor in zip(values, offset):
        if factor == 0:
            continue
        if total is None:
            total = scaled(value, factor)
        elif factor == 1:
            total = total + value
        elif factor == -1:
            total = total - value
        else:
            total = total + value * float(factor)
    return total


def bit(word, number):
    return (word & (1 << (number % bits_per_word))) != 0


def add_to(store, key, value):
    store[key] = value if store.get(key) is None else store[key] + value


def by_class(store):
    total = None
    for cls, value in store.items():
        term = value * (1.0 / math.sqrt(cls))
        total = term if total is None else total + term
    return total


def chosen(region, moduli_ref, row):
    value = jnp.where(region == 1, moduli_ref[row, 1], moduli_ref[row, 0])
    value = jnp.where(region == 2, moduli_ref[row, 2], value)
    return jnp.where(region == 3, moduli_ref[row, 3], value)


def px_at(ref, shift, x, y):
    return ref[shift + 3, pl.ds((x + 4) * SU + y + 3, 8, stride=SU), :]


def field_at(ref, field, x, y):
    return ref[field, fx_rows(x, y), :]


def crossing(y):
    found = []
    for number, offset in enumerate(OFFSETS):
        target = y + offset[1]
        if target < 0:
            found.append((number, offset, target + 3))
        elif target > 7:
            found.append((number, offset, target - 8 + 3))
    return found


def u_depth(component):
    return 6 if component == 0 else 5


def u_tile(component):
    return U_TILE + (0 if component == 0 else 1 + component * 5)


def slabs_x(
    u_hbm, w_hbm, r_hbm, odd_ref, even_ref, u_ref, w_ref, r_ref, u_sem, w_sem, r_sem
):
    parity = lax.axis_index("gx") % 2
    copies = [
        pltpu.make_async_copy(w_hbm, w_ref, w_sem),
        pltpu.make_async_copy(u_hbm, u_ref, u_sem),
        pltpu.make_async_copy(r_hbm, r_ref, r_sem),
    ]
    for copy in copies:
        copy.start()
    for copy in copies:
        copy.wait()
    for ref, right in ((even_ref, 1 - parity), (odd_ref, parity)):
        for k in range(WORDS):
            for d in range(3):
                ref[k * 3 + d] = w_ref[k, right * 5 + d].astype(F32)
        for d in range(3):
            ref[EXTRA_TILE + d] = w_ref[right * 8 + d, right + 3].astype(F32)
        for c in range(3):
            for d in range(u_depth(c)):
                ref[u_tile(c) + d] = u_ref[c, right * (8 - u_depth(c)) + d]
        for d in range(3):
            ref[R_TILE + d] = r_ref[right * 5 + d].astype(F32)


def column_sum(ux_ref, words, x, inside):
    own = [ux_ref[i * 7 + 3, ux_column(x), :] for i in range(3)]
    sums = {}
    loaded = None
    for number, offset in enumerate(OFFSETS):
        if not inside(x + offset[0]):
            continue
        if loaded != number // bits_per_word:
            loaded = number // bits_per_word
            word = words(loaded)
        difference = [
            ux_ref[i * 7 + offset[2] + 3, ux_column(x + offset[0], offset[1]), :] - own[i]
            if offset[i] != 0
            else None
            for i in range(3)
        ]
        along = combined(difference, offset)
        add_to(sums, square(offset), jnp.where(bit(word, number), along, 0.0))
    return by_class(sums)


def ratios(words, region, moduli_ref):
    counts = {}
    for k in range((WORDS + 1) // 2):
        word = words(k) if k < WORDS // 2 else words(WORDS - 1)
        group = OFFSETS[k * bits_per_word : (k + 1) * bits_per_word]
        if k < WORDS // 2:
            other = WORDS - 2 - k
            word = word | (words(other) << bits_per_word)
            group = group + OFFSETS[other * bits_per_word : (other + 1) * bits_per_word]
        else:
            group = OFFSETS[(WORDS - 1) * bits_per_word :]
        for cls in CLASSES:
            held = sum(1 << i for i, offset in enumerate(group) if square(offset) == cls)
            if held:
                add_to(counts, cls, lax.population_count(word & held))
    volume = None
    for cls in CLASSES:
        term = counts[cls].astype(F32) * math.sqrt(cls)
        volume = term if volume is None else volume + term
    inverse = 1.0 / jnp.where(volume > 0.0, volume, 1.0)
    bulk = chosen(region, moduli_ref, 0)
    shear = chosen(region, moduli_ref, 1)
    return (3.0 * inverse) * ((3.0 * bulk - 5.0 * shear) * inverse), 15.0 * shear * inverse


def spread_column(ux_ref, component, x, value):
    depth = max(-x, x - 7, 0)
    reach = 3 if depth < 4 else 2 if depth < 6 else 0
    for shift in range(-reach, reach + 1):
        ux_ref[component * 7 + shift + 3, ux_column(x), :] = rolled(value, shift)


def own_part(u_ref, w_ref, r_ref, moduli_hbm, ux_ref, own_ref, moduli_ref, moduli_sem):
    fetch = pltpu.make_async_copy(moduli_hbm, moduli_ref, moduli_sem)
    fetch.start()
    zero = jnp.zeros((8, LANES), F32)
    for i in range(3):
        for x in range(8):
            spread_column(ux_ref, i, x, u_ref[pl.ds(i * 64 + x * 8, 8), :])
        for shift in range(-2, 3):
            for y in (-3, -2, -1, 8, 9, 10):
                for x in (-6, 2, 6):
                    ux_ref[i * 7 + shift + 3, ux_rows(x, y), :] = zero
    for x in range(8):
        own_ref[x] = column_sum(
            ux_ref,
            lambda k, x=x: w_ref[pl.ds(k * 64 + x * 8, 8), :],
            x,
            lambda far: 0 <= far < 8,
        )
    fetch.wait()
    for x in range(8):
        own_ref[8 + x], own_ref[16 + x] = ratios(
            lambda k, x=x: w_ref[pl.ds(k * 64 + x * 8, 8), :],
            r_ref[pl.ds(x * 8, 8), :],
            moduli_ref,
        )


def halo_reader(even_ref, odd_ref):
    parity = lax.axis_index("gx") % 2

    def tile(index, left):
        rows = pl.ds(index * 8, 8)
        even, odd = (even_ref[rows, :], odd_ref[rows, :])
        return jnp.where(parity == 0, odd, even) if left else jnp.where(parity == 0, even, odd)

    def word(k, x):
        d = x + 3 if x < 0 else x - 8
        return tile(k * 3 + d, x < 0).astype(jnp.int32)

    def region(x):
        d = x + 3 if x < 0 else x - 8
        return tile(R_TILE + d, x < 0).astype(jnp.int32)

    return tile, word, region


def slabs_y(
    u_ref,
    w_ref,
    own_ref,
    moduli_hbm,
    even_ref,
    odd_ref,
    ux_in_ref,
    ux_ref,
    field_ref,
    odd_rows_ref,
    even_rows_ref,
    moduli_ref,
    moduli_sem,
):
    fetch = pltpu.make_async_copy(moduli_hbm, moduli_ref, moduli_sem)
    fetch.start()
    tile, halo_word, halo_region = halo_reader(even_ref, odd_ref)
    for i in range(3):
        size = u_depth(i)
        for d in range(size):
            spread_column(ux_ref, i, d - size, tile(u_tile(i) + d, True))
            spread_column(ux_ref, i, d + 8, tile(u_tile(i) + d, False))
    for x in range(8):
        value = own_ref[x]
        if x < 3 or x > 4:
            value = value + column_sum(
                ux_ref,
                lambda k, x=x: w_ref[pl.ds(k * 64 + x * 8, 8), :],
                x,
                lambda far: far < 0 or far > 7,
            )
        field_ref[0, fx_column(x), :] = value
        field_ref[1, fx_column(x), :] = own_ref[8 + x]
        field_ref[2, fx_column(x), :] = own_ref[16 + x]
    for x in (-2, -1, 8, 9):
        field_ref[0, fx_column(x), :] = column_sum(
            ux_ref, lambda k, x=x: halo_word(k, x), x, lambda far: True
        )
    fetch.wait()
    for x in (-2, -1, 8, 9):
        field_ref[1, fx_column(x), :], field_ref[2, fx_column(x), :] = ratios(
            lambda k, x=x: halo_word(k, x), halo_region(x), moduli_ref
        )
    parity_y = lax.axis_index("gy") % 2
    for ref, upward in ((odd_rows_ref, parity_y), (even_rows_ref, 1 - parity_y)):
        for depth in range(3):
            y = depth + upward * (7 - 2 * depth)
            places, field_places = slab_places(depth)
            for i in slab_components(depth):
                for x in places:
                    ref[slab_u(i, depth, x), :] = u_at(ux_ref, i, 0, x, y)
            for i in range(3):
                for x in field_places:
                    ref[slab_field(i, depth, x), :] = field_at(field_ref, i, x, y)


def fold(force, column, a, b):
    force = list(force)
    total = None
    for value in column.values():
        total = value if total is None else total + value
    for i, factor in ((0, a), (1, b)):
        if factor != 0:
            term = scaled(total, factor)
            force[i] = term if force[i] is None else force[i] + term
    for c, value in column.items():
        if c > 0:
            term = scaled(value - column[-c], c)
            force[2] = term if force[2] is None else force[2] + term
    return force


def halo_y(h):
    return h - 3 if h < 3 else h + 5


def inner_force(
    ux_ref,
    w_ref,
    r_ref,
    moduli_hbm,
    even_ref,
    odd_ref,
    field_in_ref,
    field_ref,
    wx_ref,
    part_ref,
    sum_ref,
    step_ref,
    hd_ref,
    weight_ref,
    sx_ref,
    moduli_ref,
    moduli_sem,
):
    fetch = pltpu.make_async_copy(moduli_hbm, moduli_ref, moduli_sem)
    fetch.start()
    tile, halo_word, halo_region = halo_reader(even_ref, odd_ref)
    for k in range(WORDS):
        for x in range(8):
            wx_ref[k, fx_column(x), :] = w_ref[pl.ds(k * 64 + x * 8, 8), :]
        for x in (-3, -2, -1, 8, 9, 10):
            wx_ref[k, fx_column(x), :] = halo_word(k, x)
    for d in range(3):
        wx_ref[8 + d, fx_column(-4), :] = tile(EXTRA_TILE + d, True).astype(jnp.int32)
        wx_ref[d, fx_column(11), :] = tile(EXTRA_TILE + d, False).astype(jnp.int32)
    zero = jnp.zeros((8, LANES), F32)
    for x in BLOCKS:
        for y in (-3, -2, -1, 8, 9, 10):
            for lead in range(1, 6):
                sx_ref[lead, pl.ds((x + 4) * SU + y + 3, 8, stride=SU), :] = zero
    for x in (-3, 10):
        field_ref[0, fx_column(x), :] = column_sum(
            ux_ref, lambda k, x=x: halo_word(k, x), x, lambda far: True
        )
    fetch.wait()
    for x in (-3, 10):
        field_ref[1, fx_column(x), :], field_ref[2, fx_column(x), :] = ratios(
            lambda k, x=x: halo_word(k, x), halo_region(x), moduli_ref
        )
    for y in range(8):
        step_ref[y] = time_step / chosen(r_ref[pl.ds(y, 8, stride=8), :], moduli_ref, 2)
        for x in BLOCKS:
            shear = field_at(field_ref, 2, x, y)
            for shift in range(-3, 4):
                sx_ref[
                    shift + 3, pl.ds((x + 4) * SU + y + 3, 8, stride=SU), :
                ] = rolled(shear, shift)

    for h in range(6):
        for x in (-6, 2, 6):
            hd_ref[pl.ds((x + 6) * SH + h, 8, stride=SH), :] = zero
    for x0 in BLOCKS:
        for h in range(6):
            for a in range(-2, 3):
                spread = None
                for c in range(-2, 3):
                    gathered = None
                    for y in range(8):
                        offset = (a, halo_y(h) - y, c)
                        if offset not in NUMBERS:
                            continue
                        number = NUMBERS[offset]
                        factor = 1.0 / math.sqrt(square(offset))
                        held = bit(word_at(wx_ref, number // bits_per_word, x0, y), number)
                        own = [
                            u_at(ux_ref, i, 0, x0, y) if offset[i] != 0 else None
                            for i in range(3)
                        ]
                        term = jnp.where(held, combined(own, offset) * factor, 0.0)
                        gathered = term if gathered is None else gathered + term
                    if gathered is not None:
                        value = rolled(gathered, -c)
                        spread = value if spread is None else spread + value
                if spread is not None:
                    rows = pl.ds((x0 + a + 6) * SH + h, 8, stride=SH)
                    hd_ref[rows, :] = hd_ref[rows, :] - spread

    def row(y, carry):
        own = [u_at(ux_ref, c, 0, 0, y) for c in range(3)]
        shear = px_at(sx_ref, 0, 0, y)
        force = [None, None, None]
        balance = [None, None, None]
        word = None
        column = {}
        count = {}
        for number, offset in enumerate(OFFSETS):
            if number % bits_per_word == 0:
                word = word_at(wx_ref, number // bits_per_word, 0, y)
            a, b, c = offset
            difference = [
                u_at(ux_ref, i, c, a, y + b) - own[i] if offset[i] != 0 else None
                for i in range(3)
            ]
            cls = square(offset)
            value = (shear + px_at(sx_ref, c, a, y + b)) * combined(difference, offset)
            held = bit(word, number)
            column[c] = jnp.where(held, value * (1.0 / (cls * math.sqrt(cls))), 0.0)
            count[c] = jnp.where(held, F32(1.0 / math.sqrt(cls)), F32(0.0))
            weight_ref[number * 8 + y] = count[c]
            if number + 1 == len(OFFSETS) or OFFSETS[number + 1][:2] != (a, b):
                force = fold(force, column, a, b)
                balance = fold(balance, count, a, b)
                column = {}
                count = {}
        for i in range(3):
            part_ref[i * 8 + y] = force[i]
            sum_ref[i * 8 + y] = balance[i]
        return carry

    lax.fori_loop(0, 8, row, 0)


def side_of(low, early):
    if low:
        return (0, 1, 2), -3, 4 if early else 2
    return (5, 6, 7), 3 if early else 5, 10


def add_side(
    low, early, slab_ref, ux_ref, wx_ref, field_ref, hd_ref, weight_ref, sum_ref, uh_ref, sh_ref, px_ref
):
    edge, first, last = side_of(low, early)
    halo = [(depth, 2 - depth if low else 3 + depth) for depth in range(3)]
    for depth, h in halo:
        for i in slab_components(depth):
            for x in slab_places(depth)[0]:
                value = slab_ref[slab_u(i, depth, x), :]
                for shift in range(-2, 3) if depth < 2 else (0,):
                    uh_ref[
                        i * 5 + shift + 2, pl.ds((x + 6) * SH + h, 8, stride=SH), :
                    ] = rolled(value, shift)
    for depth, h in halo:
        for x in slab_places(depth)[1]:
            part, ratio, shear = [slab_ref[slab_field(i, depth, x), :] for i in range(3)]
            pressure = (part + hd_ref[pl.ds((x + 6) * SH + h, 8, stride=SH), :]) * ratio
            for shift in range(-2, 3) if depth < 2 else (0,):
                px_ref[
                    shift + 3, pl.ds((x + 4) * SU + halo_y(h) + 3, 8, stride=SU), :
                ] = rolled(pressure, shift)
                sh_ref[shift + 2, pl.ds((x + 2) * SH + h, 8, stride=SH), :] = rolled(
                    shear, shift
                )
    for y in range(max(first, 0), min(last, 7) + 1):
        for x0 in BLOCKS:
            total = field_at(field_ref, 0, x0, y)
            if y in edge:
                sums = {}
                for number, offset, h in crossing(y):
                    far = [
                        uh_at(uh_ref, i, offset[2], x0 + offset[0], h)
                        if offset[i] != 0
                        else None
                        for i in range(3)
                    ]
                    held = bit(word_at(wx_ref, number // bits_per_word, x0, y), number)
                    add_to(sums, square(offset), jnp.where(held, combined(far, offset), 0.0))
                total = total + by_class(sums)
            pressure = total * field_at(field_ref, 1, x0, y)
            for shift in range(-3, 4):
                px_ref[
                    shift + 3, pl.ds((x0 + 4) * SU + y + 3, 8, stride=SU), :
                ] = rolled(pressure, shift)

    def row(y, force):
        force = list(force)
        if y in edge:
            own = [u_at(ux_ref, c, 0, 0, y) for c in range(3)]
            shear = field_at(field_ref, 2, 0, y)
            column = {}
            bonds = crossing(y)
            for position, (number, (a, b, c), h) in enumerate(bonds):
                offset = (a, b, c)
                far = [
                    uh_at(uh_ref, i, c, a, h) if offset[i] != 0 else None for i in range(3)
                ]
                reach = combined(far, offset)
                near = combined(
                    [own[i] if offset[i] != 0 else None for i in range(3)], offset
                )
                far_shear = sh_ref[c + 2, pl.ds((a + 2) * SH + h, 8, stride=SH), :]
                value = far_shear * (reach - near) + shear * reach
                column[c] = (value * (1.0 / square(offset))) * weight_ref[number * 8 + y]
                if position + 1 == len(bonds) or bonds[position + 1][1][:2] != (a, b):
                    force = fold(force, column, a, b)
                    column = {}
        if first <= y <= last:
            pressure = px_at(px_ref, 0, 0, y)
            force = [force[i] + pressure * sum_ref[i * 8 + y] for i in range(3)]
        column = {}
        for number, (a, b, c) in enumerate(OFFSETS):
            if not first <= y + b <= last:
                continue
            column[c] = px_at(px_ref, c, a, y + b) * weight_ref[number * 8 + y]
            if number + 1 == len(OFFSETS) or OFFSETS[number + 1][:2] != (a, b):
                force = fold(force, column, a, b)
                column = {}
        return force

    return row


def early_force(
    slab_ref,
    ux_ref,
    wx_ref,
    field_ref,
    hd_ref,
    weight_ref,
    sum_ref,
    part_ref,
    force_ref,
    uh_ref,
    sh_ref,
    px_ref,
):
    parity = lax.axis_index("gy") % 2
    shared = (ux_ref, wx_ref, field_ref, hd_ref, weight_ref, sum_ref, uh_ref, sh_ref, px_ref)
    for low in (True, False):

        @pl.when(parity == (0 if low else 1))
        def _(low=low):
            row = add_side(low, True, slab_ref, *shared)
            for y in range(8):
                force = row(y, [part_ref[i * 8 + y] for i in range(3)])
                for i in range(3):
                    force_ref[i * 8 + y] = force[i]


def outer_force(
    slab_ref,
    ux_ref,
    wx_ref,
    field_ref,
    hd_ref,
    weight_ref,
    sum_ref,
    force_ref,
    step_ref,
    u_ref,
    v_ref,
    new_u_ref,
    new_v_ref,
    uh_ref,
    sh_ref,
    px_ref,
):
    parity = lax.axis_index("gy") % 2
    shared = (ux_ref, wx_ref, field_ref, hd_ref, weight_ref, sum_ref, uh_ref, sh_ref, px_ref)
    for low in (True, False):

        @pl.when(parity == (1 if low else 0))
        def _(low=low):
            row = add_side(low, False, slab_ref, *shared)
            for y in range(8):
                force = row(y, [force_ref[i * 8 + y] for i in range(3)])
                for i in range(3):
                    rows = pl.ds(i * 64 + y, 8, stride=8)
                    velocity = v_ref[rows, :] + force[i] * step_ref[y]
                    new_v_ref[rows, :] = velocity
                    new_u_ref[rows, :] = u_ref[rows, :] + time_step * velocity


def call(body, outs, args, unplaced=(), scratch=(), flops=1000, aliases=None):
    vmem = pl.BlockSpec(memory_space=pltpu.VMEM)
    unmoved = pl.BlockSpec(memory_space=pltpu.HBM)
    return pl.pallas_call(
        body,
        out_shape=[jax.ShapeDtypeStruct(shape, dtype) for shape, dtype in outs],
        in_specs=[unmoved if position in unplaced else vmem for position in range(len(args))],
        out_specs=[vmem for _ in outs],
        scratch_shapes=scratch,
        input_output_aliases=aliases or {},
        cost_estimate=pl.CostEstimate(flops=flops, bytes_accessed=100000, transcendentals=0),
        compiler_params=pltpu.CompilerParams(vmem_limit_bytes=16 * 1024 * 1024),
    )(
        *[
            pltpu.with_memory_space_constraint(arg, pltpu.HBM) if position in unplaced else arg
            for position, arg in enumerate(args)
        ]
    )


def odd_swap(size):
    return [(i, ((i - 1) ^ 1) + 1) for i in range(1, size - 1)]


def even_swap(size):
    return [(i, i ^ 1) for i in range(size)]


def on_device(displacement, velocity, region, bond_words, moduli):
    copy = pltpu.SemaphoreType.DMA(())
    odd, even, u, words, region = call(
        slabs_x,
        [((SLAB, 8, LANES), F32)] * 2
        + [(x.shape, x.dtype) for x in (displacement, bond_words, region)],
        (displacement, bond_words, region),
        unplaced=(0, 1, 2),
        scratch=[copy, copy, copy],
    )
    size = lax.axis_size("gx")
    odd = lax.ppermute(odd, "gx", odd_swap(size))
    even = lax.ppermute(even, "gx", even_swap(size))
    even = even.reshape(SLAB * 8, LANES)
    odd = odd.reshape(SLAB * 8, LANES)
    u = u.reshape(192, LANES)
    words = words.reshape(704, LANES)
    region = region.reshape(64, LANES)
    scalars = [pltpu.SMEM(moduli.shape, F32), copy]
    displaced = ((21, UX_ROWS, LANES), F32)
    per_node = ((3, FX_ROWS, LANES), F32)
    ux, own = call(
        own_part,
        [displaced, ((24, 8, LANES), F32)],
        (u, words, region, moduli),
        unplaced=(3,),
        scratch=scalars,
        flops=10_000_000,
    )
    ux, fields, odd_rows, even_rows = call(
        slabs_y,
        [displaced, per_node, ((SLAB_Y, LANES), F32), ((SLAB_Y, LANES), F32)],
        (u, words, own, moduli, even, odd, ux),
        unplaced=(3,),
        scratch=scalars,
        flops=10_000_000,
        aliases={6: 0},
    )
    size = lax.axis_size("gy")
    odd_rows = lax.ppermute(odd_rows, "gy", odd_swap(size))
    even_rows = lax.ppermute(even_rows, "gy", even_swap(size))
    fields, wx, part, balance, step, halo, weights = call(
        inner_force,
        [
            per_node,
            ((WORDS, WX_ROWS, LANES), jnp.int32),
            ((24, 8, LANES), F32),
            ((24, 8, LANES), F32),
            ((8, 8, LANES), F32),
            ((20 * SH, LANES), F32),
            ((len(OFFSETS) * 8, 8, LANES), F32),
        ],
        (ux, words, region, moduli, even, odd, fields),
        unplaced=(3,),
        scratch=[pltpu.VMEM((7, 16 * SU, LANES), F32)] + scalars,
        flops=40_000_000,
        aliases={6: 0},
    )
    shared = (ux, wx, fields, halo, weights, balance)
    working = [
        pltpu.VMEM((15, 20 * SH, LANES), F32),
        pltpu.VMEM((5, 12 * SH, LANES), F32),
        pltpu.VMEM((7, 16 * SU, LANES), F32),
    ]
    (force,) = call(
        early_force,
        [((24, 8, LANES), F32)],
        (odd_rows,) + shared + (part,),
        scratch=working,
        flops=10_000_000,
    )
    new_u, new_v = call(
        outer_force,
        [((192, LANES), F32)] * 2,
        (even_rows,) + shared + (force, step, u, velocity.reshape(192, LANES)),
        scratch=working,
        flops=10_000_000,
    )
    return new_u.reshape(displacement.shape), new_v.reshape(velocity.shape)


def solution(mesh):
    placed = (
        P(None, "gx", "gy", None),
        P(None, "gx", "gy", None),
        P("gx", "gy", None),
        P(None, "gx", "gy", None),
        P(),
    )
    return jax.shard_map(
        on_device,
        mesh=mesh,
        in_specs=placed,
        out_specs=(P(None, "gx", "gy", None), P(None, "gx", "gy", None)),
        check_vma=False,
    )
```

```python
import math

import jax
import jax.numpy as jnp
from jax import lax
from jax.experimental import pallas as pl
from jax.experimental.pallas import tpu as pltpu
from jax.sharding import PartitionSpec as P


HORIZON = 3
time_step = 0.3
bits_per_word = 12
F32 = jnp.float32
LANES = 128

OFFSETS = [
    (a, b, c)
    for a in range(-HORIZON, HORIZON + 1)
    for b in range(-HORIZON, HORIZON + 1)
    for c in range(-HORIZON, HORIZON + 1)
    if 0 < a * a + b * b + c * c <= HORIZON * HORIZON
]
CLASSES = sorted({a * a + b * b + c * c for a, b, c in OFFSETS})
NUMBERS = {offset: number for number, offset in enumerate(OFFSETS)}
WORDS = (len(OFFSETS) + bits_per_word - 1) // bits_per_word


def square(offset):
    return offset[0] * offset[0] + offset[1] * offset[1] + offset[2] * offset[2]


UX_ROWS = 20 * 28
WX_ROWS = 16 * 18
FX_ROWS = 16 * 18
SU = 14
SH = 7
BLOCKS = (-4, 4)
EXTRA_TILE = 33
U_TILE = 36
R_TILE = 52
SLAB = 55
SLAB_Y = 218


def rolled(value, shift):
    return value if shift == 0 else pltpu.roll(value, (-shift) % LANES, 1)


def ux_rows(x, y):
    return pl.ds(((x + 6) * 14 + y + 3) * 2, 8, stride=28)


def ux_column(x, y=0):
    return pl.ds(((x + 6) * 14 + y + 3) * 2, 8, stride=2)


def fx_rows(x, y):
    return pl.ds(((x + 4) * 9 + y) * 2, 8, stride=18)


def fx_column(x):
    return pl.ds((x + 4) * 18, 8, stride=2)


def u_at(ref, component, shift, x, y):
    return ref[component * 7 + shift + 3, ux_rows(x, y), :]


def word_at(ref, k, x, y):
    return ref[k, fx_rows(x, y), :]


def uh_at(ref, component, shift, x, h):
    return ref[component * 5 + shift + 2, pl.ds((x + 6) * SH + h, 8, stride=SH), :]


def slab_u(component, depth, x):
    if depth < 2:
        return pl.ds((x + 5) * 6 + component * 2 + depth, 8, stride=6)
    return pl.ds(108 + x + 3, 8)


def slab_field(field, depth, x):
    if depth < 2:
        return pl.ds(122 + (x + 2) * 6 + field * 2 + depth, 8, stride=6)
    return pl.ds(194 + x * 3 + field, 8, stride=3)


def slab_components(depth):
    return range(3) if depth < 2 else (1,)


def slab_places(depth):
    return ((-5, 3, 5), (-2, 2)) if depth < 2 else ((-3, 3), (0,))


def scaled(value, factor):
    if factor == 1:
        return value
    if factor == -1:
        return -value
    return value * float(factor)


def combined(values, offset):
    total = None
    for value, factor in zip(values, offset):
        if factor == 0:
            continue
        if total is None:
            total = scaled(value, factor)
        elif factor == 1:
            total = total + value
        elif factor == -1:
            total = total - value
        else:
            total = total + value * float(factor)
    return total


def bit(word, number):
    return (word & (1 << (number % bits_per_word))) != 0


def add_to(store, key, value):
    store[key] = value if store.get(key) is None else store[key] + value


def by_class(store):
    total = None
    for cls, value in store.items():
        term = value * (1.0 / math.sqrt(cls))
        total = term if total is None else total + term
    return total


def chosen(region, moduli_ref, row):
    value = jnp.where(region == 1, moduli_ref[row, 1], moduli_ref[row, 0])
    value = jnp.where(region == 2, moduli_ref[row, 2], value)
    return jnp.where(region == 3, moduli_ref[row, 3], value)


def px_at(ref, shift, x, y):
    return ref[shift + 3, pl.ds((x + 4) * SU + y + 3, 8, stride=SU), :]


def field_at(ref, field, x, y):
    return ref[field, fx_rows(x, y), :]


def crossing(y):
    found = []
    for number, offset in enumerate(OFFSETS):
        target = y + offset[1]
        if target < 0:
            found.append((number, offset, target + 3))
        elif target > 7:
            found.append((number, offset, target - 8 + 3))
    return found


def u_depth(component):
    return 6 if component == 0 else 5


def u_tile(component):
    return U_TILE + (0 if component == 0 else 1 + component * 5)


def slabs_x(
    u_hbm, w_hbm, r_hbm, odd_ref, even_ref, u_ref, w_ref, r_ref, u_sem, w_sem, r_sem
):
    parity = lax.axis_index("gx") % 2
    copies = [
        pltpu.make_async_copy(w_hbm, w_ref, w_sem),
        pltpu.make_async_copy(u_hbm, u_ref, u_sem),
        pltpu.make_async_copy(r_hbm, r_ref, r_sem),
    ]
    for copy in copies:
        copy.start()
    for copy in copies:
        copy.wait()
    for ref, right in ((even_ref, 1 - parity), (odd_ref, parity)):
        for k in range(WORDS):
            for d in range(3):
                ref[k * 3 + d] = w_ref[k, right * 5 + d].astype(F32)
        for d in range(3):
            ref[EXTRA_TILE + d] = w_ref[right * 8 + d, right + 3].astype(F32)
        for c in range(3):
            for d in range(u_depth(c)):
                ref[u_tile(c) + d] = u_ref[c, right * (8 - u_depth(c)) + d]
        for d in range(3):
            ref[R_TILE + d] = r_ref[right * 5 + d].astype(F32)


def column_sum(ux_ref, words, x, inside):
    own = [ux_ref[i * 7 + 3, ux_column(x), :] for i in range(3)]
    sums = {}
    loaded = None
    for number, offset in enumerate(OFFSETS):
        if not inside(x + offset[0]):
            continue
        if loaded != number // bits_per_word:
            loaded = number // bits_per_word
            word = words(loaded)
        difference = [
            ux_ref[i * 7 + offset[2] + 3, ux_column(x + offset[0], offset[1]), :] - own[i]
            if offset[i] != 0
            else None
            for i in range(3)
        ]
        along = combined(difference, offset)
        add_to(sums, square(offset), jnp.where(bit(word, number), along, 0.0))
    return by_class(sums)


def ratios(words, region, moduli_ref):
    counts = {}
    for k in range((WORDS + 1) // 2):
        word = words(k) if k < WORDS // 2 else words(WORDS - 1)
        group = OFFSETS[k * bits_per_word : (k + 1) * bits_per_word]
        if k < WORDS // 2:
            other = WORDS - 2 - k
            word = word | (words(other) << bits_per_word)
            group = group + OFFSETS[other * bits_per_word : (other + 1) * bits_per_word]
        else:
            group = OFFSETS[(WORDS - 1) * bits_per_word :]
        for cls in CLASSES:
            held = sum(1 << i for i, offset in enumerate(group) if square(offset) == cls)
            if held:
                add_to(counts, cls, lax.population_count(word & held))
    volume = None
    for cls in CLASSES:
        term = counts[cls].astype(F32) * math.sqrt(cls)
        volume = term if volume is None else volume + term
    inverse = 1.0 / jnp.where(volume > 0.0, volume, 1.0)
    bulk = chosen(region, moduli_ref, 0)
    shear = chosen(region, moduli_ref, 1)
    return (3.0 * inverse) * ((3.0 * bulk - 5.0 * shear) * inverse), 15.0 * shear * inverse


def spread_column(ux_ref, component, x, value):
    depth = max(-x, x - 7, 0)
    reach = 3 if depth < 4 else 2 if depth < 6 else 0
    for shift in range(-reach, reach + 1):
        ux_ref[component * 7 + shift + 3, ux_column(x), :] = rolled(value, shift)


def own_part(u_ref, w_ref, r_ref, moduli_hbm, ux_ref, own_ref, moduli_ref, moduli_sem):
    fetch = pltpu.make_async_copy(moduli_hbm, moduli_ref, moduli_sem)
    fetch.start()
    zero = jnp.zeros((8, LANES), F32)
    for i in range(3):
        for x in range(8):
            spread_column(ux_ref, i, x, u_ref[pl.ds(i * 64 + x * 8, 8), :])
        for shift in range(-2, 3):
            for y in (-3, -2, -1, 8, 9, 10):
                for x in (-6, 2, 6):
                    ux_ref[i * 7 + shift + 3, ux_rows(x, y), :] = zero
    for x in range(8):
        own_ref[x] = column_sum(
            ux_ref,
            lambda k, x=x: w_ref[pl.ds(k * 64 + x * 8, 8), :],
            x,
            lambda far: 0 <= far < 8,
        )
    fetch.wait()
    for x in range(8):
        own_ref[8 + x], own_ref[16 + x] = ratios(
            lambda k, x=x: w_ref[pl.ds(k * 64 + x * 8, 8), :],
            r_ref[pl.ds(x * 8, 8), :],
            moduli_ref,
        )


def halo_reader(even_ref, odd_ref):
    parity = lax.axis_index("gx") % 2

    def tile(index, left):
        rows = pl.ds(index * 8, 8)
        even, odd = (even_ref[rows, :], odd_ref[rows, :])
        return jnp.where(parity == 0, odd, even) if left else jnp.where(parity == 0, even, odd)

    def word(k, x):
        d = x + 3 if x < 0 else x - 8
        return tile(k * 3 + d, x < 0).astype(jnp.int32)

    def region(x):
        d = x + 3 if x < 0 else x - 8
        return tile(R_TILE + d, x < 0).astype(jnp.int32)

    return tile, word, region


def slabs_y(
    u_ref,
    w_ref,
    own_ref,
    moduli_hbm,
    even_ref,
    odd_ref,
    ux_in_ref,
    ux_ref,
    field_ref,
    first_rows_ref,
    second_rows_ref,
    moduli_ref,
    moduli_sem,
):
    fetch = pltpu.make_async_copy(moduli_hbm, moduli_ref, moduli_sem)
    fetch.start()
    tile, halo_word, halo_region = halo_reader(even_ref, odd_ref)
    for i in range(3):
        size = u_depth(i)
        for d in range(size):
            spread_column(ux_ref, i, d - size, tile(u_tile(i) + d, True))
            spread_column(ux_ref, i, d + 8, tile(u_tile(i) + d, False))
    for x in range(8):
        value = own_ref[x]
        if x < 3 or x > 4:
            value = value + column_sum(
                ux_ref,
                lambda k, x=x: w_ref[pl.ds(k * 64 + x * 8, 8), :],
                x,
                lambda far: far < 0 or far > 7,
            )
        field_ref[0, fx_column(x), :] = value
        field_ref[1, fx_column(x), :] = own_ref[8 + x]
        field_ref[2, fx_column(x), :] = own_ref[16 + x]
    for x in (-2, -1, 8, 9):
        field_ref[0, fx_column(x), :] = column_sum(
            ux_ref, lambda k, x=x: halo_word(k, x), x, lambda far: True
        )
    fetch.wait()
    for x in (-2, -1, 8, 9):
        field_ref[1, fx_column(x), :], field_ref[2, fx_column(x), :] = ratios(
            lambda k, x=x: halo_word(k, x), halo_region(x), moduli_ref
        )
    parity_y = lax.axis_index("gy") % 2
    for ref, upward in ((first_rows_ref, 1 - parity_y), (second_rows_ref, parity_y)):
        for depth in range(3):
            y = depth + upward * (7 - 2 * depth)
            places, field_places = slab_places(depth)
            for i in slab_components(depth):
                for x in places:
                    ref[slab_u(i, depth, x), :] = u_at(ux_ref, i, 0, x, y)
            for i in range(3):
                for x in field_places:
                    ref[slab_field(i, depth, x), :] = field_at(field_ref, i, x, y)


def fold(force, column, a, b):
    force = list(force)
    total = None
    for value in column.values():
        total = value if total is None else total + value
    for i, factor in ((0, a), (1, b)):
        if factor != 0:
            term = scaled(total, factor)
            force[i] = term if force[i] is None else force[i] + term
    for c, value in column.items():
        if c > 0:
            term = scaled(value - column[-c], c)
            force[2] = term if force[2] is None else force[2] + term
    return force


def halo_y(h):
    return h - 3 if h < 3 else h + 5


def inner_force(
    ux_ref,
    w_ref,
    r_ref,
    moduli_hbm,
    even_ref,
    odd_ref,
    field_in_ref,
    field_ref,
    wx_ref,
    part_ref,
    sum_ref,
    step_ref,
    hd_ref,
    weight_ref,
    sx_ref,
    moduli_ref,
    moduli_sem,
):
    fetch = pltpu.make_async_copy(moduli_hbm, moduli_ref, moduli_sem)
    fetch.start()
    tile, halo_word, halo_region = halo_reader(even_ref, odd_ref)
    for k in range(WORDS):
        for x in range(8):
            wx_ref[k, fx_column(x), :] = w_ref[pl.ds(k * 64 + x * 8, 8), :]
        for x in (-3, -2, -1, 8, 9, 10):
            wx_ref[k, fx_column(x), :] = halo_word(k, x)
    for d in range(3):
        wx_ref[8 + d, fx_column(-4), :] = tile(EXTRA_TILE + d, True).astype(jnp.int32)
        wx_ref[d, fx_column(11), :] = tile(EXTRA_TILE + d, False).astype(jnp.int32)
    zero = jnp.zeros((8, LANES), F32)
    for x in BLOCKS:
        for y in (-3, -2, -1, 8, 9, 10):
            for lead in range(1, 6):
                sx_ref[lead, pl.ds((x + 4) * SU + y + 3, 8, stride=SU), :] = zero
    for x in (-3, 10):
        field_ref[0, fx_column(x), :] = column_sum(
            ux_ref, lambda k, x=x: halo_word(k, x), x, lambda far: True
        )
    fetch.wait()
    for x in (-3, 10):
        field_ref[1, fx_column(x), :], field_ref[2, fx_column(x), :] = ratios(
            lambda k, x=x: halo_word(k, x), halo_region(x), moduli_ref
        )
    for y in range(8):
        step_ref[y] = time_step / chosen(r_ref[pl.ds(y, 8, stride=8), :], moduli_ref, 2)
        for x in BLOCKS:
            shear = field_at(field_ref, 2, x, y)
            for shift in range(-3, 4):
                sx_ref[
                    shift + 3, pl.ds((x + 4) * SU + y + 3, 8, stride=SU), :
                ] = rolled(shear, shift)

    for h in range(6):
        for x in (-6, 2, 6):
            hd_ref[pl.ds((x + 6) * SH + h, 8, stride=SH), :] = zero
    for x0 in BLOCKS:
        for h in range(6):
            for a in range(-2, 3):
                spread = None
                for c in range(-2, 3):
                    gathered = None
                    for y in range(8):
                        offset = (a, halo_y(h) - y, c)
                        if offset not in NUMBERS:
                            continue
                        number = NUMBERS[offset]
                        factor = 1.0 / math.sqrt(square(offset))
                        held = bit(word_at(wx_ref, number // bits_per_word, x0, y), number)
                        own = [
                            u_at(ux_ref, i, 0, x0, y) if offset[i] != 0 else None
                            for i in range(3)
                        ]
                        term = jnp.where(held, combined(own, offset) * factor, 0.0)
                        gathered = term if gathered is None else gathered + term
                    if gathered is not None:
                        value = rolled(gathered, -c)
                        spread = value if spread is None else spread + value
                if spread is not None:
                    rows = pl.ds((x0 + a + 6) * SH + h, 8, stride=SH)
                    hd_ref[rows, :] = hd_ref[rows, :] - spread

    def row(y, carry):
        own = [u_at(ux_ref, c, 0, 0, y) for c in range(3)]
        shear = px_at(sx_ref, 0, 0, y)
        force = [None, None, None]
        balance = [None, None, None]
        word = None
        column = {}
        count = {}
        for number, offset in enumerate(OFFSETS):
            if number % bits_per_word == 0:
                word = word_at(wx_ref, number // bits_per_word, 0, y)
            a, b, c = offset
            difference = [
                u_at(ux_ref, i, c, a, y + b) - own[i] if offset[i] != 0 else None
                for i in range(3)
            ]
            cls = square(offset)
            value = (shear + px_at(sx_ref, c, a, y + b)) * combined(difference, offset)
            held = bit(word, number)
            column[c] = jnp.where(held, value * (1.0 / (cls * math.sqrt(cls))), 0.0)
            count[c] = jnp.where(held, F32(1.0 / math.sqrt(cls)), F32(0.0))
            weight_ref[number * 8 + y] = count[c]
            if number + 1 == len(OFFSETS) or OFFSETS[number + 1][:2] != (a, b):
                force = fold(force, column, a, b)
                balance = fold(balance, count, a, b)
                column = {}
                count = {}
        for i in range(3):
            part_ref[i * 8 + y] = force[i]
            sum_ref[i * 8 + y] = balance[i]
        return carry

    lax.fori_loop(0, 8, row, 0)


def side_of(low, early):
    if low:
        return (0, 1, 2), -3, 4 if early else 2
    return (5, 6, 7), 3 if early else 5, 10


def add_side(
    low, early, slab_ref, ux_ref, wx_ref, field_ref, hd_ref, weight_ref, sum_ref, uh_ref, sh_ref, px_ref
):
    edge, first, last = side_of(low, early)
    halo = [(depth, 2 - depth if low else 3 + depth) for depth in range(3)]
    for depth, h in halo:
        for i in slab_components(depth):
            for x in slab_places(depth)[0]:
                value = slab_ref[slab_u(i, depth, x), :]
                for shift in range(-2, 3) if depth < 2 else (0,):
                    uh_ref[
                        i * 5 + shift + 2, pl.ds((x + 6) * SH + h, 8, stride=SH), :
                    ] = rolled(value, shift)
    for depth, h in halo:
        for x in slab_places(depth)[1]:
            part, ratio, shear = [slab_ref[slab_field(i, depth, x), :] for i in range(3)]
            pressure = (part + hd_ref[pl.ds((x + 6) * SH + h, 8, stride=SH), :]) * ratio
            for shift in range(-2, 3) if depth < 2 else (0,):
                px_ref[
                    shift + 3, pl.ds((x + 4) * SU + halo_y(h) + 3, 8, stride=SU), :
                ] = rolled(pressure, shift)
                sh_ref[shift + 2, pl.ds((x + 2) * SH + h, 8, stride=SH), :] = rolled(
                    shear, shift
                )
    for y in range(max(first, 0), min(last, 7) + 1):
        for x0 in BLOCKS:
            total = field_at(field_ref, 0, x0, y)
            if y in edge:
                sums = {}
                for number, offset, h in crossing(y):
                    far = [
                        uh_at(uh_ref, i, offset[2], x0 + offset[0], h)
                        if offset[i] != 0
                        else None
                        for i in range(3)
                    ]
                    held = bit(word_at(wx_ref, number // bits_per_word, x0, y), number)
                    add_to(sums, square(offset), jnp.where(held, combined(far, offset), 0.0))
                total = total + by_class(sums)
            pressure = total * field_at(field_ref, 1, x0, y)
            for shift in range(-3, 4):
                px_ref[
                    shift + 3, pl.ds((x0 + 4) * SU + y + 3, 8, stride=SU), :
                ] = rolled(pressure, shift)

    def row(y, force):
        force = list(force)
        if y in edge:
            own = [u_at(ux_ref, c, 0, 0, y) for c in range(3)]
            shear = field_at(field_ref, 2, 0, y)
            column = {}
            bonds = crossing(y)
            for position, (number, (a, b, c), h) in enumerate(bonds):
                offset = (a, b, c)
                far = [
                    uh_at(uh_ref, i, c, a, h) if offset[i] != 0 else None for i in range(3)
                ]
                reach = combined(far, offset)
                near = combined(
                    [own[i] if offset[i] != 0 else None for i in range(3)], offset
                )
                far_shear = sh_ref[c + 2, pl.ds((a + 2) * SH + h, 8, stride=SH), :]
                value = far_shear * (reach - near) + shear * reach
                column[c] = (value * (1.0 / square(offset))) * weight_ref[number * 8 + y]
                if position + 1 == len(bonds) or bonds[position + 1][1][:2] != (a, b):
                    force = fold(force, column, a, b)
                    column = {}
        if first <= y <= last:
            pressure = px_at(px_ref, 0, 0, y)
            force = [force[i] + pressure * sum_ref[i * 8 + y] for i in range(3)]
        column = {}
        for number, (a, b, c) in enumerate(OFFSETS):
            if not first <= y + b <= last:
                continue
            column[c] = px_at(px_ref, c, a, y + b) * weight_ref[number * 8 + y]
            if number + 1 == len(OFFSETS) or OFFSETS[number + 1][:2] != (a, b):
                force = fold(force, column, a, b)
                column = {}
        return force

    return row


def early_force(
    slab_ref,
    ux_ref,
    wx_ref,
    field_ref,
    hd_ref,
    weight_ref,
    sum_ref,
    part_ref,
    force_ref,
    uh_ref,
    sh_ref,
    px_ref,
):
    parity = lax.axis_index("gy") % 2
    shared = (ux_ref, wx_ref, field_ref, hd_ref, weight_ref, sum_ref, uh_ref, sh_ref, px_ref)
    for low in (True, False):

        @pl.when(parity == (1 if low else 0))
        def _(low=low):
            row = add_side(low, True, slab_ref, *shared)
            for y in range(8):
                force = row(y, [part_ref[i * 8 + y] for i in range(3)])
                for i in range(3):
                    force_ref[i * 8 + y] = force[i]


def outer_force(
    slab_ref,
    ux_ref,
    wx_ref,
    field_ref,
    hd_ref,
    weight_ref,
    sum_ref,
    force_ref,
    step_ref,
    u_ref,
    v_ref,
    new_u_ref,
    new_v_ref,
    uh_ref,
    sh_ref,
    px_ref,
):
    parity = lax.axis_index("gy") % 2
    shared = (ux_ref, wx_ref, field_ref, hd_ref, weight_ref, sum_ref, uh_ref, sh_ref, px_ref)
    for low in (True, False):

        @pl.when(parity == (0 if low else 1))
        def _(low=low):
            row = add_side(low, False, slab_ref, *shared)
            for y in range(8):
                force = row(y, [force_ref[i * 8 + y] for i in range(3)])
                for i in range(3):
                    rows = pl.ds(i * 64 + y, 8, stride=8)
                    velocity = v_ref[rows, :] + force[i] * step_ref[y]
                    new_v_ref[rows, :] = velocity
                    new_u_ref[rows, :] = u_ref[rows, :] + time_step * velocity


def call(body, outs, args, unplaced=(), scratch=(), flops=1000, aliases=None):
    vmem = pl.BlockSpec(memory_space=pltpu.VMEM)
    unmoved = pl.BlockSpec(memory_space=pltpu.HBM)
    return pl.pallas_call(
        body,
        out_shape=[jax.ShapeDtypeStruct(shape, dtype) for shape, dtype in outs],
        in_specs=[unmoved if position in unplaced else vmem for position in range(len(args))],
        out_specs=[vmem for _ in outs],
        scratch_shapes=scratch,
        input_output_aliases=aliases or {},
        cost_estimate=pl.CostEstimate(flops=flops, bytes_accessed=100000, transcendentals=0),
        compiler_params=pltpu.CompilerParams(vmem_limit_bytes=16 * 1024 * 1024),
    )(
        *[
            pltpu.with_memory_space_constraint(arg, pltpu.HBM) if position in unplaced else arg
            for position, arg in enumerate(args)
        ]
    )


def odd_swap(size):
    return [(i, ((i - 1) ^ 1) + 1) for i in range(1, size - 1)]


def even_swap(size):
    return [(i, i ^ 1) for i in range(size)]


def on_device(displacement, velocity, region, bond_words, moduli):
    copy = pltpu.SemaphoreType.DMA(())
    odd, even, u, words, region = call(
        slabs_x,
        [((SLAB, 8, LANES), F32)] * 2
        + [(x.shape, x.dtype) for x in (displacement, bond_words, region)],
        (displacement, bond_words, region),
        unplaced=(0, 1, 2),
        scratch=[copy, copy, copy],
    )
    size = lax.axis_size("gx")
    odd = lax.ppermute(odd, "gx", odd_swap(size))
    even = lax.ppermute(even, "gx", even_swap(size))
    even = even.reshape(SLAB * 8, LANES)
    odd = odd.reshape(SLAB * 8, LANES)
    u = u.reshape(192, LANES)
    words = words.reshape(704, LANES)
    region = region.reshape(64, LANES)
    scalars = [pltpu.SMEM(moduli.shape, F32), copy]
    displaced = ((21, UX_ROWS, LANES), F32)
    per_node = ((3, FX_ROWS, LANES), F32)
    ux, own = call(
        own_part,
        [displaced, ((24, 8, LANES), F32)],
        (u, words, region, moduli),
        unplaced=(3,),
        scratch=scalars,
        flops=10_000_000,
    )
    ux, fields, first_rows, second_rows = call(
        slabs_y,
        [displaced, per_node, ((SLAB_Y, LANES), F32), ((SLAB_Y, LANES), F32)],
        (u, words, own, moduli, even, odd, ux),
        unplaced=(3,),
        scratch=scalars,
        flops=10_000_000,
        aliases={6: 0},
    )
    size = lax.axis_size("gy")
    first_rows = lax.ppermute(first_rows, "gy", even_swap(size))
    second_rows = lax.ppermute(second_rows, "gy", odd_swap(size))
    fields, wx, part, balance, step, halo, weights = call(
        inner_force,
        [
            per_node,
            ((WORDS, WX_ROWS, LANES), jnp.int32),
            ((24, 8, LANES), F32),
            ((24, 8, LANES), F32),
            ((8, 8, LANES), F32),
            ((20 * SH, LANES), F32),
            ((len(OFFSETS) * 8, 8, LANES), F32),
        ],
        (ux, words, region, moduli, even, odd, fields),
        unplaced=(3,),
        scratch=[pltpu.VMEM((7, 16 * SU, LANES), F32)] + scalars,
        flops=40_000_000,
        aliases={6: 0},
    )
    shared = (ux, wx, fields, halo, weights, balance)
    working = [
        pltpu.VMEM((15, 20 * SH, LANES), F32),
        pltpu.VMEM((5, 12 * SH, LANES), F32),
        pltpu.VMEM((7, 16 * SU, LANES), F32),
    ]
    (force,) = call(
        early_force,
        [((24, 8, LANES), F32)],
        (first_rows,) + shared + (part,),
        scratch=working,
        flops=10_000_000,
    )
    new_u, new_v = call(
        outer_force,
        [((192, LANES), F32)] * 2,
        (second_rows,) + shared + (force, step, u, velocity.reshape(192, LANES)),
        scratch=working,
        flops=10_000_000,
    )
    return new_u.reshape(displacement.shape), new_v.reshape(velocity.shape)


def solution(mesh):
    placed = (
        P(None, "gx", "gy", None),
        P(None, "gx", "gy", None),
        P("gx", "gy", None),
        P(None, "gx", "gy", None),
        P(),
    )
    return jax.shard_map(
        on_device,
        mesh=mesh,
        in_specs=placed,
        out_specs=(P(None, "gx", "gy", None), P(None, "gx", "gy", None)),
        check_vma=False,
    )
```
